256 devices in a mesh: parts: 2 (over y), rows: 128 (over z, x, core).
Axes of the slice: x: 4, y: 2, z: 16, core: 2. Of those that a mesh axis runs over, the one named last changes fastest.
The devices are a block of a 4x16x16 slice.
Arguments:
- latent: bfloat16 [4, 128, 160, 384], P('parts', 'rows'), parts along dimension 0, may hold values from -40 to 40
- conv_cache: bfloat16 [4, 128, 160, 384], P('parts', 'rows'), parts along dimension 0, may hold values from -6 to 6
- time_cache: bfloat16 [4, 128, 160, 384], P('parts', 'rows'), parts along dimension 0, may hold values from -6 to 6
- norm_gain: float32 [384], replicated, may hold values from 0.5 to 2
- norm_shift: float32 [384], replicated, may hold values from -3 to 3
- conv_weight: bfloat16 [3, 3, 3, 384, 384], replicated, may hold values from -0.0625 to 0.0625
- conv_bias: float32 [384], replicated, may hold values from -2 to 2
- time_weight: bfloat16 [3, 384, 768], replicated, may hold values from -0.1875 to 0.1875
- time_bias: float32 [768], replicated, may hold values from -2 to 2
- up_weight: bfloat16 [3, 3, 384, 192], replicated, may hold values from -0.109375 to 0.109375
- up_bias: float32 [192], replicated, may hold values from -2 to 2
Outputs:
- frames_out: bfloat16 [8, 256, 320, 192], P('parts', 'rows'), parts along dimension 0
The draws below stay inside these ranges and needn't reach their ends.
There are 2 independent parts, one for each index of `parts`. The reference program is written for one: setup_inputs(seed, part) draws one part's arguments, and reference() takes and returns one part's arrays. A program takes and returns all parts, laid end to end along the dimension named above; an argument that names none is the same for every part. Nothing has to cross between parts.
All inputs are finite; a program needn't handle non-finite values.
Results may differ from the reference program's by a relative error of at most 0.0056.
Values may be sent and summed in bfloat16 or wider, within the bound.
No kernel may reach another device: no remote copies, remote signals or barrier semaphores. Data moves between devices by JAX's collectives and lax.ppermute only.
A program may use at most 64 MiB of HBM per device.

```python
import math
import jax
import jax.numpy as jnp
from jax import lax

C = 384
C_OUT = 192
GROUPS = 32
FRAMES = 2
WIDE = 160
HEIGHT = 128


def draw_latent(key, part):
    key_base = jax.random.fold_in(key, 11)
    key_chan = jax.random.fold_in(key, 12)
    position = jnp.arange(HEIGHT, dtype=jnp.float32) / max(HEIGHT - 1, 1)
    chan_scale = 0.3 * 10.0 ** jax.random.uniform(key_chan, (C,), jnp.float32)
    base = jnp.clip(jax.random.normal(key_base, (FRAMES, HEIGHT, WIDE, C), jnp.float32), -4.0, 4.0)
    row_scale = 0.3 * 10.0 ** position
    values = base * row_scale[None, :, None, None] * chan_scale
    return values.astype(jnp.bfloat16)


def block_levels(key, extent, shards, least, top_value):
    level = 1.0
    for dim, parts in shards:
        draws = jax.random.uniform(jax.random.fold_in(jax.random.fold_in(key, 6), dim), (parts,), jnp.float32, least / len(shards), top_value / len(shards))
        level = level * jnp.repeat(jnp.exp(draws), extent[dim] // parts).reshape((-1,) + (1,) * (len(extent) - 1 - dim))
    return level


def bell_draw(rng, extent, deviation, bound, split=(), held_as=jnp.bfloat16):
    array = deviation * jax.random.normal(rng, extent, jnp.float32)
    if split:
        array = array * block_levels(rng, extent, split, -0.22, 0.18)
    return jnp.clip(array, -bound, bound).astype(held_as)


def setup_inputs(seed: int = 0, part: int = 0) -> dict:
    key_list = jax.random.split(jax.random.key(seed), 12)
    part_keys = jax.random.split(jax.random.fold_in(key_list[11], part), 12)
    return {
        "latent": draw_latent(jax.random.fold_in(jax.random.fold_in(key_list[11], part), 71), part),
        "conv_cache": bell_draw(part_keys[1], (2, HEIGHT, WIDE, C), 1.0, 6.0, ((1, 128),)),
        "time_cache": bell_draw(part_keys[2], (2, HEIGHT, WIDE, C), 1.0, 6.0, ((1, 128),)),
        "norm_gain": jnp.clip(jnp.exp(jax.random.uniform(key_list[3], (C,), jnp.float32, math.log(0.5), math.log(2.0))), 0.5, 2.0),
        "norm_shift": bell_draw(key_list[4], (C,), 0.5, 3.0, (), jnp.float32),
        "conv_weight": bell_draw(key_list[5], (3, 3, 3, C, C), (27 * C) ** -0.5, 0.0625),
        "conv_bias": bell_draw(key_list[6], (C,), 0.3, 2.0, (), jnp.float32),
        "time_weight": bell_draw(key_list[7], (3, C, 2 * C), (3 * C) ** -0.5, 0.1875),
        "time_bias": bell_draw(key_list[8], (2 * C,), 0.3, 2.0, (), jnp.float32),
        "up_weight": bell_draw(key_list[9], (3, 3, C, C_OUT), (9 * C) ** -0.5, 0.109375),
        "up_bias": bell_draw(key_list[10], (C_OUT,), 0.3, 2.0, (), jnp.float32),
    }


EPSILON = 1e-06

def normalize(signal, norm_gain, norm_shift):
    frame_count, row_count, col_count, channels = signal.shape
    grouped = signal.reshape(frame_count, row_count, col_count, GROUPS, channels // GROUPS)
    center = lax.optimization_barrier(jnp.mean(grouped, axis=(0, 1, 2, 4), keepdims=True))
    spread = lax.optimization_barrier(jnp.mean(jnp.square(grouped - center), axis=(0, 1, 2, 4), keepdims=True))
    normed = ((grouped - center) * lax.rsqrt(spread + EPSILON)).reshape(signal.shape)
    return jax.nn.silu(normed * norm_gain + norm_shift).astype(jnp.bfloat16)

def conv_taps(padded, kernel, row_count, col_count):
    channels = padded.shape[-1]
    total = jnp.zeros((padded.shape[0] * row_count * col_count, kernel.shape[-1]), jnp.float32)
    for row_tap in range(3):
        window = jnp.concatenate([padded[:, row_tap:row_tap + row_count, col_tap:col_tap + col_count] for col_tap in range(3)], axis=-1)
        total = total + jnp.dot(window.reshape(-1, 3 * channels), kernel[row_tap].reshape(3 * channels, -1), preferred_element_type=jnp.float32)
    return total

def temporal(block, time_cache, time_weight, time_bias):
    frame_count = block.shape[0]
    channels = block.shape[-1]
    joined = jnp.concatenate([time_cache, block], axis=0)
    window = jnp.concatenate([joined[frame_tap:frame_tap + frame_count] for frame_tap in range(3)], axis=-1)
    mixed = jnp.dot(window.reshape(-1, 3 * channels), time_weight.reshape(3 * channels, -1), preferred_element_type=jnp.float32) + time_bias
    mixed = mixed.astype(jnp.bfloat16).reshape(block.shape[:-1] + (2, channels))
    return jnp.moveaxis(mixed, 3, 1).reshape((2 * frame_count,) + block.shape[1:])

def reference(latent, conv_cache, time_cache, norm_gain, norm_shift, conv_weight, conv_bias, time_weight, time_bias, up_weight, up_bias):
    frame_count, row_count, col_count, channels = latent.shape
    signal = latent.astype(jnp.float32)
    active = normalize(signal, norm_gain, norm_shift)
    joined = jnp.concatenate([conv_cache, active], axis=0)
    padded = jnp.pad(joined, ((0, 0), (1, 1), (1, 1), (0, 0)))
    summed = conv_bias + jnp.zeros((frame_count * row_count * col_count, channels), jnp.float32)
    for frame_tap in range(3):
        summed = summed + conv_taps(padded[frame_tap:frame_tap + frame_count], conv_weight[frame_tap], row_count, col_count)
    block = (signal + summed.reshape(signal.shape)).astype(jnp.bfloat16)
    doubled = temporal(block, time_cache, time_weight, time_bias)
    upsampled = jnp.repeat(jnp.repeat(doubled, 2, axis=1), 2, axis=2)
    padded_up = jnp.pad(upsampled, ((0, 0), (1, 1), (1, 1), (0, 0)))

    def one_frame(frame):
        result = conv_taps(frame[None], up_weight, 2 * row_count, 2 * col_count) + up_bias
        return result.astype(jnp.bfloat16).reshape(2 * row_count, 2 * col_count, -1)
    return lax.map(one_frame, padded_up)
```

```python
import jax
import jax.numpy as jnp
from jax import lax
from jax.sharding import PartitionSpec as P

GROUPS = 32
ROWS = "rows"
EPSILON = 1e-06


def sum_over_rows(value):
    spread_out = jnp.broadcast_to(value, (lax.axis_size(ROWS),) + value.shape)
    return jnp.sum(lax.all_to_all(spread_out, ROWS, 0, 0), axis=0)


def neighbours(value):
    devices = lax.axis_size(ROWS)
    up = [(i, i + 1) for i in range(devices - 1)]
    down = [(j, i) for i, j in up]
    return lax.ppermute(value, ROWS, up), lax.ppermute(value, ROWS, down)


def conv_taps(padded, kernel, row_count, col_count):
    channels = padded.shape[-1]
    total = jnp.zeros((padded.shape[0] * row_count * col_count, kernel.shape[-1]), jnp.float32)
    for row_tap in range(3):
        window = jnp.concatenate(
            [
                padded[:, row_tap : row_tap + row_count, col_tap : col_tap + col_count]
                for col_tap in range(3)
            ],
            axis=-1,
        )
        total = total + jnp.dot(
            window.reshape(-1, 3 * channels),
            kernel[row_tap].reshape(3 * channels, -1),
            preferred_element_type=jnp.float32,
        )
    return total


def temporal(block, time_cache, time_weight, time_bias):
    frame_count = block.shape[0]
    channels = block.shape[-1]
    joined = jnp.concatenate([time_cache, block], axis=0)
    window = jnp.concatenate(
        [joined[frame_tap : frame_tap + frame_count] for frame_tap in range(3)], axis=-1
    )
    mixed = (
        jnp.dot(
            window.reshape(-1, 3 * channels),
            time_weight.reshape(3 * channels, -1),
            preferred_element_type=jnp.float32,
        )
        + time_bias
    )
    mixed = mixed.astype(jnp.bfloat16).reshape(block.shape[:-1] + (2, channels))
    return jnp.moveaxis(mixed, 3, 1).reshape((2 * frame_count,) + block.shape[1:])


def on_device(
    latent,
    conv_cache,
    time_cache,
    norm_gain,
    norm_shift,
    conv_weight,
    conv_bias,
    time_weight,
    time_bias,
    up_weight,
    up_bias,
):
    frame_count, row_count, col_count, channels = latent.shape
    me, devices = lax.axis_index(ROWS), lax.axis_size(ROWS)
    raw = jnp.concatenate([latent, conv_cache], axis=0)
    raw_before, raw_after = neighbours(raw)
    signal = latent.astype(jnp.float32)
    grouped = signal.reshape(frame_count, row_count, col_count, GROUPS, channels // GROUPS)
    entries = float(frame_count * row_count * devices * col_count * (channels // GROUPS))
    sums = jnp.concatenate(
        [jnp.sum(grouped, axis=(0, 1, 2, 4)), jnp.sum(grouped * grouped, axis=(0, 1, 2, 4))]
    )
    sums = sum_over_rows(sums)
    center = sums[:GROUPS] / entries
    spread = sums[GROUPS:] / entries - center * center
    center = jnp.repeat(center, channels // GROUPS)
    scale = jnp.repeat(lax.rsqrt(spread + EPSILON), channels // GROUPS)
    raw = jnp.concatenate([raw_before, raw, raw_after], axis=1)
    wide = raw[:frame_count].astype(jnp.float32)
    active = jax.nn.silu((wide - center) * scale * norm_gain + norm_shift).astype(jnp.bfloat16)
    row = me * row_count + lax.broadcasted_iota(jnp.int32, (1, row_count + 2, 1, 1), 1)
    inside = (row >= 1) & (row <= devices * row_count)
    active = jnp.where(inside, active, jnp.zeros_like(active))
    joined = jnp.concatenate([raw[frame_count:], active], axis=0)
    padded = jnp.pad(joined, ((0, 0), (0, 0), (1, 1), (0, 0)))
    summed = conv_bias + jnp.zeros((frame_count * row_count * col_count, channels), jnp.float32)
    for frame_tap in range(3):
        summed = summed + conv_taps(
            padded[frame_tap : frame_tap + frame_count],
            conv_weight[frame_tap],
            row_count,
            col_count,
        )
    block = (signal + summed.reshape(signal.shape)).astype(jnp.bfloat16)
    doubled = temporal(block, time_cache, time_weight, time_bias)
    before, after = neighbours(doubled)
    upsampled = jnp.concatenate([before, doubled, doubled, after], axis=1)
    upsampled = jnp.repeat(upsampled, 2, axis=2)
    padded_up = jnp.pad(upsampled, ((0, 0), (0, 0), (1, 1), (0, 0)))
    result = conv_taps(padded_up, up_weight, 2 * row_count, 2 * col_count) + up_bias
    return result.astype(jnp.bfloat16).reshape(
        2 * frame_count, 2 * row_count, 2 * col_count, up_weight.shape[-1]
    )


def solution(mesh):
    placed = P("parts", ROWS, None, None)
    return jax.shard_map(
        on_device,
        mesh=mesh,
        in_specs=(placed,) * 3 + (P(),) * 8,
        out_specs=placed,
        check_vma=False,
    )
```

```python
import functools

import jax
import jax.numpy as jnp
from jax import lax
from jax.experimental import pallas as pl
from jax.experimental.pallas import tpu as pltpu
from jax.sharding import PartitionSpec as P

GROUPS = 32
ROWS = "rows"
EPSILON = 1e-06
LANES = 128
F32 = jnp.float32
BF16 = jnp.bfloat16
ALL_VMEM = 67043328
VMEM = pl.BlockSpec(memory_space=pltpu.VMEM)
HBM = pl.BlockSpec(memory_space=pltpu.HBM)
SMEM = pl.BlockSpec(memory_space=pltpu.SMEM)


def group_matrix(channels, first, flip):
    size = channels // GROUPS
    shape = (LANES, channels) if flip else (channels, LANES)
    lane = lax.broadcasted_iota(jnp.int32, shape, 0 if flip else 1) - first
    channel = lax.broadcasted_iota(jnp.int32, shape, 1 if flip else 0)
    return ((channel >= lane * size) & (channel < lane * size + size) & (lane >= 0)).astype(F32)


def exact_dot(a, b):
    return jnp.dot(a, b, preferred_element_type=F32, precision=lax.Precision.HIGHEST)


def pack_kernel(latent, conv_cache, time_cache, near, far, sums, sems):
    frames, _, _, channels = latent.shape
    jobs = []
    for n, source in enumerate((latent, conv_cache, time_cache)):
        for t in range(frames):
            jobs.append((source.at[t, 0], near.at[n * frames + t]))
            if n < 2:
                jobs.append((source.at[t, 0], far.at[n * frames + t]))
    copies = [pltpu.make_async_copy(a, b, sems.at[i]) for i, (a, b) in enumerate(jobs)]
    for copy in copies:
        copy.start()
    total = jnp.zeros((8, channels), F32)
    square = jnp.zeros((8, channels), F32)
    for t in range(frames):
        copies[2 * t].wait()
        wide = near[t].astype(F32).reshape(-1, 8, channels)
        total = total + jnp.sum(wide, axis=0)
        square = square + jnp.sum(wide * wide, axis=0)
    grouped = exact_dot(total, group_matrix(channels, 0, False))
    grouped = grouped + exact_dot(square, group_matrix(channels, GROUPS, False))
    row = jnp.sum(grouped, axis=0, keepdims=True)
    sums[...] = jnp.broadcast_to(row[None], sums.shape)
    for copy in copies[1 : 2 * frames : 2] + copies[2 * frames :]:
        copy.wait()


def shifted(value, step):
    length = value.shape[0]
    rolled = pltpu.roll(value, (-step) % length, 0)
    row = lax.broadcasted_iota(jnp.int32, value.shape, 0)
    return jnp.where((row + step >= 0) & (row + step < length), rolled, 0.0)


def main_kernel(entries, place, *refs):
    n_in = 10
    far_refs, out = refs[:n_in], refs[n_in]
    near_refs, (taps, acc, time_taps, up_taps, sems) = refs[n_in + 1 : 2 * n_in + 1], refs[2 * n_in + 1 :]
    stats, vectors, own, before, after, before_far, after_far, weight, time_weight, up_weight = near_refs
    channels = own.shape[-1]
    width = own.shape[1]
    frames = own.shape[0] // 3
    copies = []
    for n in range(n_in):
        if n != 7:
            copies.append(pltpu.make_async_copy(far_refs[n], near_refs[n], sems.at[n]))
    taps_in = []
    for c in range(3):
        for a in range(3):
            for b in range(3):
                rows = pl.ds((a * 3 + b) * channels, channels)
                taps_in.append(
                    pltpu.make_async_copy(
                        far_refs[7].at[a, b, c], weight.at[c, rows, :], sems.at[n_in + len(taps_in)]
                    )
                )
    for copy in copies[:7] + taps_in + copies[7:]:
        copy.start()
    copies[0].wait()
    copies[1].wait()
    gain, shift, conv_bias = (vectors[n : n + 1, :channels] for n in range(3))
    time_bias, up_bias = vectors[3:4, :], vectors[4:5, : 2 * out.shape[-2]]
    me, last = place[0], place[1]
    total = jnp.sum(stats[:, 0, :], axis=0, keepdims=True)
    total = jnp.broadcast_to(total, (8, LANES))
    center = exact_dot(total, group_matrix(channels, 0, True))[:1] / entries
    spread = exact_dot(total, group_matrix(channels, GROUPS, True))[:1] / entries
    spread = spread - center * center
    scale = lax.rsqrt(spread + EPSILON) * gain
    offset = shift

    sources = (before_far, before, own, after, after_far)
    rows_of = lambda t, r: pl.ds((t * 3 + r) * width, width)

    def place_row(frame, r, value):
        for a in range(3):
            t = frame - a
            if 0 <= t < frames:
                for b in range(3):
                    if 0 <= r - b < 3:
                        k = (a * 3 + b) * channels
                        taps[rows_of(t, r - b), k : k + channels] = value

    for copy in copies[2:7]:
        copy.wait()
    for r in range(5):
        row = me + (r - 2)
        inside = ((row >= 0) & (row <= last)).astype(F32)
        for t in range(frames):
            place_row(t, r, sources[r][frames + t])
            value = sources[r][t].astype(F32)
            value = (value - center) * scale + offset
            value = value / (1.0 + jnp.exp(-value)) * inside
            place_row(frames + t, r, value.astype(BF16))

    for c in range(3):
        for copy in taps_in[c * 9 : c * 9 + 9]:
            copy.wait()
        acc[c] = jnp.dot(taps[...], weight[c], preferred_element_type=F32)

    for r in range(3):
        for t in range(frames):
            rows = rows_of(t, r)
            value = acc[1, rows, :] + shifted(acc[0, rows, :], -1) + shifted(acc[2, rows, :], 1)
            value = value + conv_bias + sources[r + 1][t].astype(F32)
            block = value.astype(BF16)
            cached = sources[r + 1][2 * frames + t]
            for frame, item in ((t, cached), (frames + t, block)):
                for a in range(3):
                    if 0 <= frame - a < frames:
                        k = a * channels
                        time_taps[rows_of(frame - a, r), k : k + channels] = item

    copies[7].wait()
    for t in range(frames):
        for r in range(3):
            row = me + (r - 1)
            inside = ((row >= 0) & (row <= last)).astype(F32)
            weights = time_weight[...].reshape(3 * channels, 2 * channels)
            mixed = jnp.dot(time_taps[rows_of(t, r), :], weights, preferred_element_type=F32)
            mixed = ((mixed + time_bias) * inside).astype(BF16)
            for k in range(2):
                part = mixed[:, k * channels : (k + 1) * channels]
                lines = pl.ds((2 * t + k) * width, width)
                for p in range(2):
                    if 0 <= r - p < 2:
                        up_taps[p, lines, (r - p) * channels : (r - p + 1) * channels] = part

    copies[8].wait()
    outputs = out.shape[-2]
    lane = lax.broadcasted_iota(jnp.int32, (width, 2 * outputs), 1)
    low = lax.broadcasted_iota(jnp.int32, (width, 2 * width), 0)
    high = lax.broadcasted_iota(jnp.int32, (width, 2 * width), 1)
    spread_even = (high == 2 * low).astype(F32).astype(BF16)
    spread_odd = (high == 2 * low + 1).astype(F32).astype(BF16)
    for f in range(2 * frames):
        for p in range(2):
            lines = pl.ds(f * width, width)
            value = dot_nt(up_taps[p, lines, :], up_weight[p])
            inner, outer = value[:, : 2 * outputs], value[:, 2 * outputs :]
            outer = jnp.where(lane < outputs, shifted(outer, -1), shifted(outer, 1))
            value = (inner + outer + up_bias).T.astype(BF16)
            even = jnp.dot(value[:outputs], spread_even, preferred_element_type=F32)
            odd = jnp.dot(value[outputs:], spread_odd, preferred_element_type=F32)
            out[f, p] = (even + odd).astype(BF16)


def dot_nt(a, b):
    return lax.dot_general(a, b, (((1,), (1,)), ((), ())), preferred_element_type=F32)


def small_kernel(up_weight, gain, shift, conv_bias, time_bias, up_bias, out, vectors):
    outputs, channels = up_weight.shape[2:]
    for n, item in enumerate((gain, shift, conv_bias)):
        vectors[n : n + 1, :channels] = item[...].reshape(1, -1)
    vectors[3:4, :] = time_bias[...].reshape(1, -1)
    vectors[4:5, :outputs] = up_bias[...].reshape(1, -1)
    vectors[4:5, outputs : 2 * outputs] = up_bias[...].reshape(1, -1)
    columns = lambda b: [up_weight[b, c].astype(F32) for c in range(3)]
    first, middle, final = columns(0), columns(1), columns(2)
    add = lambda u, v: [x + y for x, y in zip(u, v)]
    by_row = ((first, add(middle, final)), (add(first, middle), final))
    for p in range(2):
        for j in range(2):
            v = by_row[p][j]
            for n, item in enumerate((v[1] + v[2], v[0] + v[1], v[0], v[2])):
                rows = pl.ds(n * outputs, outputs)
                out[p, rows, j * channels : (j + 1) * channels] = item.astype(BF16)


def moved(value, step):
    devices = lax.axis_size(ROWS)
    pairs = [(i, i + step) for i in range(devices) if 0 <= i + step < devices]
    return lax.ppermute(value, ROWS, pairs)


def on_device(
    latent,
    conv_cache,
    time_cache,
    norm_gain,
    norm_shift,
    conv_weight,
    conv_bias,
    time_weight,
    time_bias,
    up_weight,
    up_bias,
):
    frames, row_count, width, channels = latent.shape
    outputs = up_weight.shape[-1]
    me, devices = lax.axis_index(ROWS), lax.axis_size(ROWS)
    near, far, sums = pl.pallas_call(
        pack_kernel,
        out_shape=(
            jax.ShapeDtypeStruct((3 * frames, width, channels), BF16),
            jax.ShapeDtypeStruct((2 * frames, width, channels), BF16),
            jax.ShapeDtypeStruct((devices, 1, LANES), F32),
        ),
        in_specs=[HBM] * 3,
        out_specs=(VMEM,) * 3,
        scratch_shapes=[pltpu.SemaphoreType.DMA((5 * frames,))],
        compiler_params=pltpu.CompilerParams(vmem_limit_bytes=ALL_VMEM),
        cost_estimate=pl.CostEstimate(flops=2**21, bytes_accessed=2**21, transcendentals=0),
        name="pack",
    )(latent, conv_cache, time_cache)
    before_far, after_far = moved(far, 2), moved(far, -2)
    before, after = moved(near, 1), moved(near, -1)
    stats = lax.all_to_all(sums, ROWS, 0, 0)
    entries = float(frames * row_count * devices * width * (channels // GROUPS))
    place = jnp.stack([me, jnp.int32(devices - 1)]).astype(jnp.int32)
    subpixel, vectors = pl.pallas_call(
        small_kernel,
        out_shape=(
            jax.ShapeDtypeStruct((2, 4 * outputs, 2 * channels), BF16),
            jax.ShapeDtypeStruct((8, 2 * channels), F32),
        ),
        in_specs=[VMEM] * 6,
        out_specs=(VMEM, VMEM),
        compiler_params=pltpu.CompilerParams(vmem_limit_bytes=ALL_VMEM),
        cost_estimate=pl.CostEstimate(flops=2**21, bytes_accessed=2**22, transcendentals=0),
        name="small",
    )(jnp.swapaxes(up_weight, 2, 3), norm_gain, norm_shift, conv_bias, time_bias, up_bias)
    inputs = (stats, vectors, near, before, after, before_far, after_far, conv_weight, time_weight, subpixel)
    flops = 2 * frames * 3 * width * channels * channels * 27
    out = pl.pallas_call(
        functools.partial(main_kernel, entries),
        out_shape=jax.ShapeDtypeStruct((2 * frames, 2, outputs, 2 * width), BF16),
        in_specs=[SMEM] + [HBM] * 10,
        out_specs=VMEM,
        scratch_shapes=[
            *[pltpu.VMEM(item.shape, item.dtype) for item in inputs[:7]],
            pltpu.VMEM((3, 9 * channels, channels), BF16),
            *[pltpu.VMEM(item.shape, item.dtype) for item in inputs[8:]],
            pltpu.VMEM((frames * 3 * width, 9 * channels), BF16),
            pltpu.VMEM((3, frames * 3 * width, channels), F32),
            pltpu.VMEM((frames * 3 * width, 3 * channels), BF16),
            pltpu.VMEM((2, 2 * frames * width, 2 * channels), BF16),
            pltpu.SemaphoreType.DMA((len(inputs) + 27,)),
        ],
        compiler_params=pltpu.CompilerParams(vmem_limit_bytes=ALL_VMEM),
        cost_estimate=pl.CostEstimate(flops=flops, bytes_accessed=2**24, transcendentals=2**20),
        name="decode",
    )(place, *inputs)
    return jnp.swapaxes(out, 2, 3)


def solution(mesh):
    placed = P("parts", ROWS, None, None)
    return jax.shard_map(
        on_device,
        mesh=mesh,
        in_specs=(placed,) * 3 + (P(),) * 8,
        out_specs=placed,
        check_vma=False,
    )
```

```python
import functools

import jax
import jax.numpy as jnp
from jax import lax
from jax.experimental import pallas as pl
from jax.experimental.pallas import tpu as pltpu
from jax.sharding import PartitionSpec as P

GROUPS = 32
ROWS = "rows"
EPSILON = 1e-06
LANES = 128
F32 = jnp.float32
BF16 = jnp.bfloat16
ALL_VMEM = 67043328
VMEM = pl.BlockSpec(memory_space=pltpu.VMEM)
HBM = pl.BlockSpec(memory_space=pltpu.HBM)
SMEM = pl.BlockSpec(memory_space=pltpu.SMEM)


def group_matrix(channels, first, flip):
    size = channels // GROUPS
    shape = (LANES, channels) if flip else (channels, LANES)
    lane = lax.broadcasted_iota(jnp.int32, shape, 0 if flip else 1) - first
    channel = lax.broadcasted_iota(jnp.int32, shape, 1 if flip else 0)
    return ((channel >= lane * size) & (channel < lane * size + size) & (lane >= 0)).astype(F32)


def exact_dot(a, b):
    return jnp.dot(a, b, preferred_element_type=F32, precision=lax.Precision.HIGHEST)


def pack_kernel(latent, conv_cache, time_cache, near, sums, sems):
    frames, _, _, channels = latent.shape
    jobs = []
    for n, source in enumerate((latent, conv_cache, time_cache)):
        for t in range(frames):
            jobs.append((source.at[t, 0], near.at[n * frames + t]))
    copies = [pltpu.make_async_copy(a, b, sems.at[i]) for i, (a, b) in enumerate(jobs)]
    for copy in copies:
        copy.start()
    total = jnp.zeros((8, channels), F32)
    square = jnp.zeros((8, channels), F32)
    for t in range(frames):
        copies[t].wait()
        wide = near[t].astype(F32).reshape(-1, 8, channels)
        total = total + jnp.sum(wide, axis=0)
        square = square + jnp.sum(wide * wide, axis=0)
    grouped = exact_dot(total, group_matrix(channels, 0, False))
    grouped = grouped + exact_dot(square, group_matrix(channels, GROUPS, False))
    row = jnp.sum(grouped, axis=0, keepdims=True)
    sums[...] = jnp.broadcast_to(row[None], sums.shape)
    for copy in copies[frames:]:
        copy.wait()


def shifted(value, step):
    length = value.shape[0]
    rolled = pltpu.roll(value, (-step) % length, 0)
    row = lax.broadcasted_iota(jnp.int32, value.shape, 0)
    return jnp.where((row + step >= 0) & (row + step < length), rolled, 0.0)


def start_copies(refs, sems):
    copies = [pltpu.make_async_copy(a, b, sems.at[n]) for n, (a, b) in enumerate(refs)]
    for copy in copies:
        copy.start()
    return copies


def conv_kernel(entries, place, *refs):
    far_refs, weight_far, out = refs[:5], refs[5], refs[6]
    near_refs, (weight, taps, acc, sems) = refs[7:12], refs[12:]
    stats, vectors, own, before, after = near_refs
    channels = own.shape[-1]
    width = own.shape[1]
    frames = own.shape[0] // 3
    moves = list(zip(far_refs, near_refs))
    for c in range(3):
        for a in range(3):
            for b in range(3):
                rows = pl.ds((a * 3 + b) * channels, channels)
                moves.append((weight_far.at[a, b, c], weight.at[c, rows, :]))
    copies = start_copies(moves, sems)
    copies[0].wait()
    copies[1].wait()
    gain, shift, conv_bias = (vectors[n : n + 1, :channels] for n in range(3))
    total = jnp.sum(stats[:, 0, :], axis=0, keepdims=True)
    total = jnp.broadcast_to(total, (8, LANES))
    center = exact_dot(total, group_matrix(channels, 0, True))[:1] / entries
    spread = exact_dot(total, group_matrix(channels, GROUPS, True))[:1] / entries
    spread = spread - center * center
    scale = lax.rsqrt(spread + EPSILON) * gain

    def place_row(frame, b, value):
        for a in range(3):
            t = frame - a
            if 0 <= t < frames:
                k = (a * 3 + b) * channels
                taps[t * width : (t + 1) * width, k : k + channels] = value

    for copy in copies[2:5]:
        copy.wait()
    for b, source in enumerate((before, own, after)):
        row = place[0] + (b - 1)
        inside = ((row >= 0) & (row <= place[1])).astype(F32)
        for t in range(frames):
            place_row(t, b, source[frames + t])
            value = source[t].astype(F32)
            value = (value - center) * scale + shift
            value = value / (1.0 + jnp.exp(-value)) * inside
            place_row(frames + t, b, value.astype(BF16))

    for c in range(3):
        for copy in copies[5 + c * 9 : 14 + c * 9]:
            copy.wait()
        acc[c] = jnp.dot(taps[...], weight[c], preferred_element_type=F32)

    for t in range(frames):
        rows = pl.ds(t * width, width)
        value = acc[1, rows, :] + shifted(acc[0, rows, :], -1) + shifted(acc[2, rows, :], 1)
        value = value + conv_bias + own[t].astype(F32)
        out[t] = value.astype(BF16)


def up_kernel(place, *refs):
    far_refs, out = refs[:9], refs[9]
    near_refs, (time_taps, mixed, up_taps, lifted, turned, sems) = refs[10:19], refs[19:]
    own, before, after, block, block_before, block_after, vectors, time_weight, up_weight = near_refs
    frames, width, channels = block.shape
    outputs = out.shape[-2]
    moves = [(a, b) for a, b in zip(far_refs, near_refs)]
    for n in range(3):
        moves[n] = (far_refs[n].at[pl.ds(2 * frames, frames)], near_refs[n])
    copies = start_copies(moves, sems)
    for copy in copies[:6]:
        copy.wait()
    rows_of = lambda t, r: pl.ds((t * 3 + r) * width, width)
    sources = ((before, block_before), (own, block), (after, block_after))
    for r in range(3):
        for t in range(frames):
            for frame, item in ((t, sources[r][0][t]), (frames + t, sources[r][1][t])):
                for a in range(3):
                    if 0 <= frame - a < frames:
                        k = a * channels
                        time_taps[rows_of(frame - a, r), k : k + channels] = item
    copies[6].wait()
    copies[7].wait()
    time_bias, up_bias = vectors[3:4, :], vectors[4:5, : 2 * outputs]
    weights = time_weight[...].reshape(3 * channels, 2 * channels)
    mixed[...] = jnp.dot(time_taps[...], weights, preferred_element_type=F32)
    for r in range(3):
        row = place[0] + (r - 1)
        inside = ((row >= 0) & (row <= place[1])).astype(F32)
        for t in range(frames):
            value = ((mixed[rows_of(t, r), :] + time_bias) * inside).astype(BF16)
            for k in range(2):
                part = value[:, k * channels : (k + 1) * channels]
                lines = pl.ds((2 * t + k) * width, width)
                for p in range(2):
                    if 0 <= r - p < 2:
                        up_taps[p, lines, (r - p) * channels : (r - p + 1) * channels] = part

    copies[8].wait()
    lane = lax.broadcasted_iota(jnp.int32, (width, 2 * outputs), 1)
    low = lax.broadcasted_iota(jnp.int32, (width, 2 * width), 0)
    high = lax.broadcasted_iota(jnp.int32, (width, 2 * width), 1)
    spread_out = [(high == 2 * low + q).astype(F32).astype(BF16) for q in range(2)]
    for p in range(2):
        lifted[...] = dot_nt(up_taps[p], up_weight[p])
        for f in range(2 * frames):
            lines = pl.ds(f * width, width)
            inner, outer = lifted[lines, : 2 * outputs], lifted[lines, 2 * outputs :]
            outer = jnp.where(lane < outputs, shifted(outer, -1), shifted(outer, 1))
            value = (inner + outer + up_bias).T.astype(BF16)
            for q in range(2):
                turned[q, pl.ds(f * outputs, outputs), :] = value[q * outputs : (q + 1) * outputs]
        value = jnp.dot(turned[0], spread_out[0], preferred_element_type=F32)
        value = value + jnp.dot(turned[1], spread_out[1], preferred_element_type=F32)
        out[:, p] = value.astype(BF16).reshape(2 * frames, outputs, 2 * width)


def dot_nt(a, b):
    return lax.dot_general(a, b, (((1,), (1,)), ((), ())), preferred_element_type=F32)


def small_kernel(up_weight, gain, shift, conv_bias, time_bias, up_bias, out, vectors):
    outputs, channels = up_weight.shape[2:]
    for n, item in enumerate((gain, shift, conv_bias)):
        vectors[n : n + 1, :channels] = item[...].reshape(1, -1)
    vectors[3:4, :] = time_bias[...].reshape(1, -1)
    vectors[4:5, :outputs] = up_bias[...].reshape(1, -1)
    vectors[4:5, outputs : 2 * outputs] = up_bias[...].reshape(1, -1)
    columns = lambda b: [up_weight[b, c].astype(F32) for c in range(3)]
    first, middle, final = columns(0), columns(1), columns(2)
    add = lambda u, v: [x + y for x, y in zip(u, v)]
    by_row = ((first, add(middle, final)), (add(first, middle), final))
    for p in range(2):
        for j in range(2):
            v = by_row[p][j]
            for n, item in enumerate((v[1] + v[2], v[0] + v[1], v[0], v[2])):
                rows = pl.ds(n * outputs, outputs)
                out[p, rows, j * channels : (j + 1) * channels] = item.astype(BF16)


def moved(value, step):
    devices = lax.axis_size(ROWS)
    pairs = [(i, i + step) for i in range(devices) if 0 <= i + step < devices]
    return lax.ppermute(value, ROWS, pairs)


def on_device(
    latent,
    conv_cache,
    time_cache,
    norm_gain,
    norm_shift,
    conv_weight,
    conv_bias,
    time_weight,
    time_bias,
    up_weight,
    up_bias,
):
    frames, row_count, width, channels = latent.shape
    outputs = up_weight.shape[-1]
    me, devices = lax.axis_index(ROWS), lax.axis_size(ROWS)
    near, sums = pl.pallas_call(
        pack_kernel,
        out_shape=(
            jax.ShapeDtypeStruct((3 * frames, width, channels), BF16),
            jax.ShapeDtypeStruct((devices, 1, LANES), F32),
        ),
        in_specs=[HBM] * 3,
        out_specs=(VMEM,) * 2,
        scratch_shapes=[pltpu.SemaphoreType.DMA((3 * frames,))],
        compiler_params=pltpu.CompilerParams(vmem_limit_bytes=ALL_VMEM),
        cost_estimate=pl.CostEstimate(flops=2**21, bytes_accessed=2**21, transcendentals=0),
        name="pack",
    )(latent, conv_cache, time_cache)
    before, after = moved(near, 1), moved(near, -1)
    stats = lax.all_to_all(sums, ROWS, 0, 0)
    entries = float(frames * row_count * devices * width * (channels // GROUPS))
    place = jnp.stack([me, jnp.int32(devices - 1)]).astype(jnp.int32)
    subpixel, vectors = pl.pallas_call(
        small_kernel,
        out_shape=(
            jax.ShapeDtypeStruct((2, 4 * outputs, 2 * channels), BF16),
            jax.ShapeDtypeStruct((8, 2 * channels), F32),
        ),
        in_specs=[VMEM] * 6,
        out_specs=(VMEM, VMEM),
        compiler_params=pltpu.CompilerParams(vmem_limit_bytes=ALL_VMEM),
        cost_estimate=pl.CostEstimate(flops=2**21, bytes_accessed=2**22, transcendentals=0),
        name="small",
    )(jnp.swapaxes(up_weight, 2, 3), norm_gain, norm_shift, conv_bias, time_bias, up_bias)
    params = pltpu.CompilerParams(vmem_limit_bytes=ALL_VMEM)
    copy_of = lambda item: pltpu.VMEM(item.shape, item.dtype)
    inputs = (stats, vectors, near, before, after)
    pixels = frames * width
    block = pl.pallas_call(
        functools.partial(conv_kernel, entries),
        out_shape=jax.ShapeDtypeStruct((frames, width, channels), BF16),
        in_specs=[SMEM] + [HBM] * 6,
        out_specs=VMEM,
        scratch_shapes=[
            *[copy_of(item) for item in inputs],
            pltpu.VMEM((3, 9 * channels, channels), BF16),
            pltpu.VMEM((pixels, 9 * channels), BF16),
            pltpu.VMEM((3, pixels, channels), F32),
            pltpu.SemaphoreType.DMA((32,)),
        ],
        compiler_params=params,
        cost_estimate=pl.CostEstimate(
            flops=2 * pixels * 27 * channels * channels, bytes_accessed=2**24, transcendentals=2**20
        ),
        name="conv",
    )(place, *inputs, conv_weight)
    caches = (near, before, after)
    inputs = (block, moved(block, 1), moved(block, -1), vectors, time_weight, subpixel)
    out = pl.pallas_call(
        up_kernel,
        out_shape=jax.ShapeDtypeStruct((2 * frames, 2, outputs, 2 * width), BF16),
        in_specs=[SMEM] + [HBM] * 9,
        out_specs=VMEM,
        scratch_shapes=[
            *[copy_of(block) for _ in caches],
            *[copy_of(item) for item in inputs],
            pltpu.VMEM((3 * pixels, 3 * channels), BF16),
            pltpu.VMEM((3 * pixels, 2 * channels), F32),
            pltpu.VMEM((2, 2 * pixels, 2 * channels), BF16),
            pltpu.VMEM((2 * pixels, 4 * outputs), F32),
            pltpu.VMEM((2, 2 * frames * outputs, width), BF16),
            pltpu.SemaphoreType.DMA((9,)),
        ],
        compiler_params=params,
        cost_estimate=pl.CostEstimate(
            flops=8 * pixels * 4 * channels * outputs * 2, bytes_accessed=2**23, transcendentals=0
        ),
        name="up",
    )(place, *caches, *inputs)
    return jnp.swapaxes(out, 2, 3)


def solution(mesh):
    placed = P("parts", ROWS, None, None)
    return jax.shard_map(
        on_device,
        mesh=mesh,
        in_specs=(placed,) * 3 + (P(),) * 8,
        out_specs=placed,
        check_vma=False,
    )
```

```python
import functools

import jax
import jax.numpy as jnp
from jax import lax
from jax.experimental import pallas as pl
from jax.experimental.pallas import tpu as pltpu
from jax.sharding import PartitionSpec as P

GROUPS = 32
ROWS = "rows"
EPSILON = 1e-06
LANES = 128
F32 = jnp.float32
BF16 = jnp.bfloat16
ALL_VMEM = 67043328
CONV_VMEM = 50 * 2**20
UP_VMEM = 24 * 2**20
VMEM = pl.BlockSpec(memory_space=pltpu.VMEM)
HBM = pl.BlockSpec(memory_space=pltpu.HBM)


def group_matrix(channels, first, flip):
    size = channels // GROUPS
    shape = (LANES, channels) if flip else (channels, LANES)
    lane = lax.broadcasted_iota(jnp.int32, shape, 0 if flip else 1) - first
    channel = lax.broadcasted_iota(jnp.int32, shape, 1 if flip else 0)
    return ((channel >= lane * size) & (channel < lane * size + size) & (lane >= 0)).astype(F32)


def exact_dot(a, b):
    return jnp.dot(a, b, preferred_element_type=F32, precision=lax.Precision.HIGHEST)


def pack_kernel(latent, conv_cache, time_cache, near, sums, sems):
    frames, _, _, channels = latent.shape
    jobs = []
    for n, source in enumerate((latent, conv_cache, time_cache)):
        for t in range(frames):
            jobs.append((source.at[t, 0], near.at[n * frames + t]))
    copies = [pltpu.make_async_copy(a, b, sems.at[i]) for i, (a, b) in enumerate(jobs)]
    for copy in copies:
        copy.start()
    total = jnp.zeros((8, channels), F32)
    square = jnp.zeros((8, channels), F32)
    for t in range(frames):
        copies[t].wait()
        wide = near[t].astype(F32).reshape(-1, 8, channels)
        total = total + jnp.sum(wide, axis=0)
        square = square + jnp.sum(wide * wide, axis=0)
    grouped = exact_dot(total, group_matrix(channels, 0, False))
    grouped = grouped + exact_dot(square, group_matrix(channels, GROUPS, False))
    row = jnp.sum(grouped, axis=0, keepdims=True)
    sums[...] = jnp.broadcast_to(row[None], sums.shape)
    for copy in copies[frames:]:
        copy.wait()


def shifted(value, step):
    length = value.shape[0]
    rolled = pltpu.roll(value, (-step) % length, 0)
    row = lax.broadcasted_iota(jnp.int32, value.shape, 0)
    return jnp.where((row + step >= 0) & (row + step < length), rolled, 0.0)


def inside_image(step):
    row = lax.axis_index(ROWS) + step
    return ((row >= 0) & (row < lax.axis_size(ROWS))).astype(F32)


def row_at(b, own, partner, outer, frame):
    if b == 1:
        return own[frame]
    even = lax.axis_index(ROWS) % 2 == 0
    first, second = (outer, partner) if b == 0 else (partner, outer)
    return jnp.where(even, first[frame], second[frame])


def start_copies(refs, sems):
    copies = [pltpu.make_async_copy(a, b, sems.at[n]) for n, (a, b) in enumerate(refs)]
    for copy in copies:
        copy.start()
    return copies


def conv_kernel(entries, stats, vectors, own, partner, outer, weight_far, out, weight, taps, acc, sems):
    channels = own.shape[-1]
    width = own.shape[1]
    frames = own.shape[0] // 3
    moves = []
    for c in range(3):
        for a in range(3):
            for b in range(3):
                rows = pl.ds((a * 3 + b) * channels, channels)
                moves.append((weight_far.at[a, b, c], weight.at[c, rows, :]))
    copies = start_copies(moves, sems)
    gain, shift, conv_bias = (vectors[:, n * channels : (n + 1) * channels] for n in range(3))
    total = jnp.sum(stats[:, 0, :], axis=0, keepdims=True)
    total = jnp.broadcast_to(total, (8, LANES))
    center = exact_dot(total, group_matrix(channels, 0, True))[:1] / entries
    spread = exact_dot(total, group_matrix(channels, GROUPS, True))[:1] / entries
    spread = spread - center * center
    scale = lax.rsqrt(spread + EPSILON) * gain

    def place_row(frame, b, value):
        for a in range(3):
            t = frame - a
            if 0 <= t < frames:
                k = (a * 3 + b) * channels
                taps[t * width : (t + 1) * width, k : k + channels] = value

    for b in range(3):
        inside = inside_image(b - 1)
        for t in range(frames):
            place_row(t, b, row_at(b, own, partner, outer, frames + t))
            value = row_at(b, own, partner, outer, t).astype(F32)
            value = (value - center) * scale + shift
            value = value / (1.0 + jnp.exp(-value)) * inside
            place_row(frames + t, b, value.astype(BF16))

    for c in range(3):
        for copy in copies[9 * c : 9 * c + 9]:
            copy.wait()
        acc[c] = jnp.dot(taps[...], weight[c], preferred_element_type=F32)

    for t in range(frames):
        rows = pl.ds(t * width, width)
        value = acc[1, rows, :] + shifted(acc[0, rows, :], -1) + shifted(acc[2, rows, :], 1)
        value = value + conv_bias + own[t].astype(F32)
        out[t] = value.astype(BF16)


def up_kernel(
    own,
    partner,
    outer,
    block,
    block_partner,
    block_outer,
    vectors,
    time_weight,
    up_weight,
    out,
    time_taps,
    mixed,
    up_taps,
    lifted,
    turned,
):
    frames, width, channels = block.shape
    outputs = out.shape[-2]
    rows_of = lambda t, r: pl.ds((t * 3 + r) * width, width)
    for r in range(3):
        for t in range(frames):
            cached = row_at(r, own, partner, outer, 2 * frames + t)
            for frame, item in ((t, cached), (frames + t, row_at(r, block, block_partner, block_outer, t))):
                for a in range(3):
                    if 0 <= frame - a < frames:
                        k = a * channels
                        time_taps[rows_of(frame - a, r), k : k + channels] = item
    time_bias = vectors[:, 3 * channels : 5 * channels]
    up_bias = vectors[:, 5 * channels :]
    weights = time_weight[...].reshape(3 * channels, 2 * channels)
    mixed[...] = jnp.dot(time_taps[...], weights, preferred_element_type=F32)
    for r in range(3):
        inside = inside_image(r - 1)
        for t in range(frames):
            value = ((mixed[rows_of(t, r), :] + time_bias) * inside).astype(BF16)
            for k in range(2):
                part = value[:, k * channels : (k + 1) * channels]
                lines = pl.ds((2 * t + k) * width, width)
                for p in range(2):
                    if 0 <= r - p < 2:
                        up_taps[p, lines, (r - p) * channels : (r - p + 1) * channels] = part

    lane = lax.broadcasted_iota(jnp.int32, (width, 2 * outputs), 1)
    low = lax.broadcasted_iota(jnp.int32, (width, 2 * width), 0)
    high = lax.broadcasted_iota(jnp.int32, (width, 2 * width), 1)
    spread_out = [(high == 2 * low + q).astype(F32).astype(BF16) for q in range(2)]
    for p in range(2):
        lifted[...] = dot_nt(up_taps[p], up_weight[p])
        for f in range(2 * frames):
            lines = pl.ds(f * width, width)
            inner, outer = lifted[lines, : 2 * outputs], lifted[lines, 2 * outputs :]
            outer = jnp.where(lane < outputs, shifted(outer, -1), shifted(outer, 1))
            value = (inner + outer + up_bias).T.astype(BF16)
            for q in range(2):
                turned[q, pl.ds(f * outputs, outputs), :] = value[q * outputs : (q + 1) * outputs]
        value = jnp.dot(turned[0], spread_out[0], preferred_element_type=F32)
        value = value + jnp.dot(turned[1], spread_out[1], preferred_element_type=F32)
        out[:, p] = value.astype(BF16).reshape(2 * frames, outputs, 2 * width)


def dot_nt(a, b):
    return lax.dot_general(a, b, (((1,), (1,)), ((), ())), preferred_element_type=F32)


def subpixel_kernel(up_weight, out):
    outputs, channels = up_weight.shape[2:]
    columns = lambda b: [up_weight[b, c].astype(F32) for c in range(3)]
    first, middle, final = columns(0), columns(1), columns(2)
    add = lambda u, v: [x + y for x, y in zip(u, v)]
    by_row = ((first, add(middle, final)), (add(first, middle), final))
    for p in range(2):
        for j in range(2):
            v = by_row[p][j]
            for n, item in enumerate((v[1] + v[2], v[0] + v[1], v[0], v[2])):
                rows = pl.ds(n * outputs, outputs)
                out[p, rows, j * channels : (j + 1) * channels] = item.astype(BF16)


def swapped(value):
    devices = lax.axis_size(ROWS)
    across = [(i, i - 1 if i % 2 == 0 else i + 1) for i in range(devices)]
    across = [(i, j) for i, j in across if 0 <= j < devices]
    outer = lax.ppermute(value, ROWS, across)
    return lax.ppermute(value, ROWS, [(i, i ^ 1) for i in range(devices)]), outer


def on_device(
    latent,
    conv_cache,
    time_cache,
    norm_gain,
    norm_shift,
    conv_weight,
    conv_bias,
    time_weight,
    time_bias,
    up_weight,
    up_bias,
):
    frames, row_count, width, channels = latent.shape
    outputs = up_weight.shape[-1]
    devices = lax.axis_size(ROWS)
    near, sums = pl.pallas_call(
        pack_kernel,
        out_shape=(
            jax.ShapeDtypeStruct((3 * frames, width, channels), BF16),
            jax.ShapeDtypeStruct((devices, 1, LANES), F32),
        ),
        in_specs=[HBM] * 3,
        out_specs=(VMEM,) * 2,
        scratch_shapes=[pltpu.SemaphoreType.DMA((3 * frames,))],
        compiler_params=pltpu.CompilerParams(vmem_limit_bytes=ALL_VMEM),
        cost_estimate=pl.CostEstimate(flops=2**21, bytes_accessed=2**21, transcendentals=0),
        name="pack",
    )(latent, conv_cache, time_cache)
    partner, outer = swapped(near)
    stats = lax.all_to_all(sums, ROWS, 0, 0)
    entries = float(frames * row_count * devices * width * (channels // GROUPS))
    subpixel = pl.pallas_call(
        subpixel_kernel,
        out_shape=jax.ShapeDtypeStruct((2, 4 * outputs, 2 * channels), BF16),
        in_specs=[VMEM],
        out_specs=VMEM,
        compiler_params=pltpu.CompilerParams(vmem_limit_bytes=12 * 2**20),
        cost_estimate=pl.CostEstimate(flops=2**21, bytes_accessed=2**24, transcendentals=0),
        name="subpixel",
    )(jnp.swapaxes(up_weight, 2, 3))
    vectors = jnp.concatenate([norm_gain, norm_shift, conv_bias, time_bias, up_bias, up_bias])
    vectors = vectors.reshape(1, -1)
    pixels = frames * width
    block = pl.pallas_call(
        functools.partial(conv_kernel, entries),
        out_shape=jax.ShapeDtypeStruct((frames, width, channels), BF16),
        in_specs=[VMEM] * 5 + [HBM],
        out_specs=VMEM,
        scratch_shapes=[
            pltpu.VMEM((3, 9 * channels, channels), BF16),
            pltpu.VMEM((pixels, 9 * channels), BF16),
            pltpu.VMEM((3, pixels, channels), F32),
            pltpu.SemaphoreType.DMA((27,)),
        ],
        compiler_params=pltpu.CompilerParams(vmem_limit_bytes=CONV_VMEM),
        cost_estimate=pl.CostEstimate(
            flops=2 * pixels * 27 * channels * channels, bytes_accessed=2**24, transcendentals=2**20
        ),
        name="conv",
    )(stats, vectors, near, partner, outer, conv_weight)
    inputs = (near, partner, outer, block, *swapped(block), vectors, time_weight, subpixel)
    out = pl.pallas_call(
        up_kernel,
        out_shape=jax.ShapeDtypeStruct((2 * frames, 2, outputs, 2 * width), BF16),
        in_specs=[VMEM] * 9,
        out_specs=VMEM,
        scratch_shapes=[
            pltpu.VMEM((3 * pixels, 3 * channels), BF16),
            pltpu.VMEM((3 * pixels, 2 * channels), F32),
            pltpu.VMEM((2, 2 * pixels, 2 * channels), BF16),
            pltpu.VMEM((2 * pixels, 4 * outputs), F32),
            pltpu.VMEM((2, 2 * frames * outputs, width), BF16),
        ],
        compiler_params=pltpu.CompilerParams(vmem_limit_bytes=UP_VMEM),
        cost_estimate=pl.CostEstimate(
            flops=8 * pixels * 4 * channels * outputs * 2, bytes_accessed=2**23, transcendentals=0
        ),
        name="up",
    )(*inputs)
    return jnp.swapaxes(out, 2, 3)


def solution(mesh):
    placed = P("parts", ROWS, None, None)
    return jax.shard_map(
        on_device,
        mesh=mesh,
        in_specs=(placed,) * 3 + (P(),) * 8,
        out_specs=placed,
        check_vma=False,
    )
```

```python
import functools

import jax
import jax.numpy as jnp
from jax import lax
from jax.experimental import pallas as pl
from jax.experimental.pallas import tpu as pltpu
from jax.sharding import PartitionSpec as P

GROUPS = 32
ROWS = "rows"
EPSILON = 1e-06
LANES = 128
F32 = jnp.float32
BF16 = jnp.bfloat16
ALL_VMEM = 67043328
CACHED_VMEM = 44 * 2**20
CONV_VMEM = 50 * 2**20
UP_VMEM = 24 * 2**20
VMEM = pl.BlockSpec(memory_space=pltpu.VMEM)
HBM = pl.BlockSpec(memory_space=pltpu.HBM)


def group_matrix(channels, first, flip):
    size = channels // GROUPS
    shape = (LANES, channels) if flip else (channels, LANES)
    lane = lax.broadcasted_iota(jnp.int32, shape, 0 if flip else 1) - first
    channel = lax.broadcasted_iota(jnp.int32, shape, 1 if flip else 0)
    return ((channel >= lane * size) & (channel < lane * size + size) & (lane >= 0)).astype(F32)


def exact_dot(a, b):
    return jnp.dot(a, b, preferred_element_type=F32, precision=lax.Precision.HIGHEST)


def pack_kernel(latent, conv_cache, time_cache, near, sums, sems):
    frames, _, _, channels = latent.shape
    jobs = []
    for n, source in enumerate((latent, conv_cache, time_cache)):
        for t in range(frames):
            jobs.append((source.at[t, 0], near.at[n * frames + t]))
    copies = [pltpu.make_async_copy(a, b, sems.at[i]) for i, (a, b) in enumerate(jobs)]
    for copy in copies:
        copy.start()
    total = jnp.zeros((8, channels), F32)
    square = jnp.zeros((8, channels), F32)
    for t in range(frames):
        copies[t].wait()
        wide = near[t].astype(F32).reshape(-1, 8, channels)
        total = total + jnp.sum(wide, axis=0)
        square = square + jnp.sum(wide * wide, axis=0)
    grouped = exact_dot(total, group_matrix(channels, 0, False))
    grouped = grouped + exact_dot(square, group_matrix(channels, GROUPS, False))
    row = jnp.sum(grouped, axis=0, keepdims=True)
    sums[...] = jnp.broadcast_to(row[None], sums.shape)
    for copy in copies[frames:]:
        copy.wait()


def shifted(value, step):
    length = value.shape[0]
    rolled = pltpu.roll(value, (-step) % length, 0)
    row = lax.broadcasted_iota(jnp.int32, value.shape, 0)
    return jnp.where((row + step >= 0) & (row + step < length), rolled, 0.0)


def inside_image(step):
    row = lax.axis_index(ROWS) + step
    return ((row >= 0) & (row < lax.axis_size(ROWS))).astype(F32)


def row_at(b, own, partner, outer, frame):
    if b == 1:
        return own[frame]
    even = lax.axis_index(ROWS) % 2 == 0
    first, second = (outer, partner) if b == 0 else (partner, outer)
    return jnp.where(even, first[frame], second[frame])


def start_copies(refs, sems):
    copies = [pltpu.make_async_copy(a, b, sems.at[n]) for n, (a, b) in enumerate(refs)]
    for copy in copies:
        copy.start()
    return copies


def weight_copies(weight_far, weight, taken, sems):
    channels = weight.shape[-1]
    moves = []
    for c in range(3):
        for n, a in enumerate(taken):
            for b in range(3):
                rows = pl.ds(b * channels, channels)
                moves.append((weight_far.at[a, b, c], weight.at[c, n, rows, :]))
    return start_copies(moves, sems)


def tap_sums(copies, taps, weight, acc, shared, single, rows):
    source, target = rows
    for c in range(3):
        for copy in copies[6 * c : 6 * c + 6]:
            copy.wait()
        acc[c] = jnp.dot(taps[...], weight[c, shared], preferred_element_type=F32)
        more = jnp.dot(taps[source, :], weight[c, single], preferred_element_type=F32)
        acc[c, target, :] = acc[c, target, :] + more


def joined_columns(acc, rows):
    return acc[1, rows, :] + shifted(acc[0, rows, :], -1) + shifted(acc[2, rows, :], 1)


def cached_kernel(vectors, own, partner, outer, weight_far, out, weight, taps, acc, sems):
    width, channels = own.shape[1:]
    copies = weight_copies(weight_far, weight, (0, 1), sems)
    first, second = pl.ds(0, width), pl.ds(width, width)
    for b in range(3):
        for t, lines in enumerate((first, second)):
            taps[lines, b * channels : (b + 1) * channels] = row_at(b, own, partner, outer, 2 + t)
    tap_sums(copies, taps, weight, acc, 0, 1, (second, first))
    conv_bias = vectors[:, 2 * channels : 3 * channels]
    for t, lines in enumerate((first, second)):
        latent = own[t].astype(F32)
        out[t] = joined_columns(acc, lines) + conv_bias + latent
        out[2 + t] = latent


def conv_kernel(entries, stats, vectors, own, partner, outer, weight_far, out, weight, taps, acc, sems):
    width, channels = own.shape[1:]
    copies = weight_copies(weight_far, weight, (1, 2), sems)
    gain, shift = (vectors[:, n * channels : (n + 1) * channels] for n in range(2))
    total = jnp.sum(stats[:, 0, :], axis=0, keepdims=True)
    total = jnp.broadcast_to(total, (8, LANES))
    center = exact_dot(total, group_matrix(channels, 0, True))[:1] / entries
    spread = exact_dot(total, group_matrix(channels, GROUPS, True))[:1] / entries
    spread = spread - center * center
    scale = lax.rsqrt(spread + EPSILON) * gain
    first, second = pl.ds(0, width), pl.ds(width, width)
    for b in range(3):
        inside = inside_image(b - 1)
        for t, lines in enumerate((first, second)):
            value = own[2 + t] if b == 1 else row_at(b, own, partner, outer, t).astype(F32)
            value = (value - center) * scale + shift
            value = value / (1.0 + jnp.exp(-value)) * inside
            taps[lines, b * channels : (b + 1) * channels] = value.astype(BF16)
    tap_sums(copies, taps, weight, acc, 1, 0, (first, second))
    for t, lines in enumerate((first, second)):
        out[t] = (joined_columns(acc, lines) + own[t]).astype(BF16)


def up_kernel(
    own,
    partner,
    outer,
    block,
    block_partner,
    block_outer,
    vectors,
    time_weight,
    up_weight,
    far_out,
    out,
    time_taps,
    mixed,
    up_taps,
    lifted,
    turned,
    sems,
):
    frames, width, channels = block.shape
    outputs = out.shape[-2]
    copies = []
    rows_of = lambda t, r: pl.ds((t * 3 + r) * width, width)
    for r in range(3):
        for t in range(frames):
            cached = row_at(r, own, partner, outer, 2 * frames + t)
            for frame, item in ((t, cached), (frames + t, row_at(r, block, block_partner, block_outer, t))):
                for a in range(3):
                    if 0 <= frame - a < frames:
                        k = a * channels
                        time_taps[rows_of(frame - a, r), k : k + channels] = item
    time_bias = vectors[:, 3 * channels : 5 * channels]
    up_bias = vectors[:, 5 * channels :]
    weights = time_weight[...].reshape(3 * channels, 2 * channels)
    mixed[...] = jnp.dot(time_taps[...], weights, preferred_element_type=F32)
    for r in range(3):
        inside = inside_image(r - 1)
        for t in range(frames):
            value = ((mixed[rows_of(t, r), :] + time_bias) * inside).astype(BF16)
            for k in range(2):
                part = value[:, k * channels : (k + 1) * channels]
                lines = pl.ds((2 * t + k) * width, width)
                for p in range(2):
                    if 0 <= r - p < 2:
                        up_taps[p, lines, (r - p) * channels : (r - p + 1) * channels] = part

    lane = lax.broadcasted_iota(jnp.int32, (width, 2 * outputs), 1)
    low = lax.broadcasted_iota(jnp.int32, (width, 2 * width), 0)
    high = lax.broadcasted_iota(jnp.int32, (width, 2 * width), 1)
    spread_out = [(high == 2 * low + q).astype(F32).astype(BF16) for q in range(2)]
    for p in range(2):
        lifted[...] = dot_nt(up_taps[p], up_weight[p])
        for f in range(2 * frames):
            lines = pl.ds(f * width, width)
            inner, outer = lifted[lines, : 2 * outputs], lifted[lines, 2 * outputs :]
            outer = jnp.where(lane < outputs, shifted(outer, -1), shifted(outer, 1))
            value = (inner + outer + up_bias).T.astype(BF16)
            for q in range(2):
                turned[q, pl.ds(f * outputs, outputs), :] = value[q * outputs : (q + 1) * outputs]
        value = jnp.dot(turned[0], spread_out[0], preferred_element_type=F32)
        value = value + jnp.dot(turned[1], spread_out[1], preferred_element_type=F32)
        out[p] = value.astype(BF16).reshape(2 * frames, outputs, 2 * width)
        copies.append(pltpu.make_async_copy(out.at[p], far_out.at[:, p], sems.at[p]))
        copies[p].start()
    for copy in copies:
        copy.wait()


def dot_nt(a, b):
    return lax.dot_general(a, b, (((1,), (1,)), ((), ())), preferred_element_type=F32)


def subpixel_kernel(up_weight, out):
    outputs, channels = up_weight.shape[2:]
    columns = lambda b: [up_weight[b, c].astype(F32) for c in range(3)]
    first, middle, final = columns(0), columns(1), columns(2)
    add = lambda u, v: [x + y for x, y in zip(u, v)]
    by_row = ((first, add(middle, final)), (add(first, middle), final))
    for p in range(2):
        for j in range(2):
            v = by_row[p][j]
            for n, item in enumerate((v[1] + v[2], v[0] + v[1], v[0], v[2])):
                rows = pl.ds(n * outputs, outputs)
                out[p, rows, j * channels : (j + 1) * channels] = item.astype(BF16)


def swapped(value):
    devices = lax.axis_size(ROWS)
    across = [(i, i - 1 if i % 2 == 0 else i + 1) for i in range(devices)]
    across = [(i, j) for i, j in across if 0 <= j < devices]
    outer = lax.ppermute(value, ROWS, across)
    return lax.ppermute(value, ROWS, [(i, i ^ 1) for i in range(devices)]), outer


def on_device(
    latent,
    conv_cache,
    time_cache,
    norm_gain,
    norm_shift,
    conv_weight,
    conv_bias,
    time_weight,
    time_bias,
    up_weight,
    up_bias,
):
    frames, row_count, width, channels = latent.shape
    outputs = up_weight.shape[-1]
    devices = lax.axis_size(ROWS)
    near, sums = pl.pallas_call(
        pack_kernel,
        out_shape=(
            jax.ShapeDtypeStruct((3 * frames, width, channels), BF16),
            jax.ShapeDtypeStruct((devices, 1, LANES), F32),
        ),
        in_specs=[HBM] * 3,
        out_specs=(VMEM,) * 2,
        scratch_shapes=[pltpu.SemaphoreType.DMA((3 * frames,))],
        compiler_params=pltpu.CompilerParams(vmem_limit_bytes=ALL_VMEM),
        cost_estimate=pl.CostEstimate(flops=2**21, bytes_accessed=2**21, transcendentals=0),
        name="pack",
    )(latent, conv_cache, time_cache)
    partner, outer = swapped(near)
    stats = lax.all_to_all(sums, ROWS, 0, 0)
    entries = float(frames * row_count * devices * width * (channels // GROUPS))
    subpixel = pl.pallas_call(
        subpixel_kernel,
        out_shape=jax.ShapeDtypeStruct((2, 4 * outputs, 2 * channels), BF16),
        in_specs=[VMEM],
        out_specs=VMEM,
        compiler_params=pltpu.CompilerParams(vmem_limit_bytes=12 * 2**20),
        cost_estimate=pl.CostEstimate(flops=2**21, bytes_accessed=2**24, transcendentals=0),
        name="subpixel",
    )(jnp.swapaxes(up_weight, 2, 3))
    vectors = jnp.concatenate([norm_gain, norm_shift, conv_bias, time_bias, up_bias, up_bias])
    vectors = vectors.reshape(1, -1)
    pixels = frames * width
    flops = pixels * 27 * channels * channels
    scratch = [
        pltpu.VMEM((3, 2, 3 * channels, channels), BF16),
        pltpu.VMEM((pixels, 3 * channels), BF16),
        pltpu.VMEM((3, pixels, channels), F32),
        pltpu.SemaphoreType.DMA((18,)),
    ]
    base = pl.pallas_call(
        cached_kernel,
        out_shape=jax.ShapeDtypeStruct((2 * frames, width, channels), F32),
        in_specs=[VMEM] * 4 + [HBM],
        out_specs=VMEM,
        scratch_shapes=scratch,
        compiler_params=pltpu.CompilerParams(vmem_limit_bytes=CACHED_VMEM),
        cost_estimate=pl.CostEstimate(flops=flops, bytes_accessed=2**23, transcendentals=0),
        name="cached",
    )(vectors, near, partner, outer, conv_weight)
    block = pl.pallas_call(
        functools.partial(conv_kernel, entries),
        out_shape=jax.ShapeDtypeStruct((frames, width, channels), BF16),
        in_specs=[VMEM] * 5 + [HBM],
        out_specs=VMEM,
        scratch_shapes=scratch,
        compiler_params=pltpu.CompilerParams(vmem_limit_bytes=CONV_VMEM),
        cost_estimate=pl.CostEstimate(flops=flops, bytes_accessed=2**23, transcendentals=2**18),
        name="conv",
    )(stats, vectors, base, partner, outer, conv_weight)
    inputs = (near, partner, outer, block, *swapped(block), vectors, time_weight, subpixel)
    out = pl.pallas_call(
        up_kernel,
        out_shape=jax.ShapeDtypeStruct((2 * frames, 2, outputs, 2 * width), BF16),
        in_specs=[VMEM] * 9,
        out_specs=HBM,
        scratch_shapes=[
            pltpu.VMEM((2, 2 * frames, outputs, 2 * width), BF16),
            pltpu.VMEM((3 * pixels, 3 * channels), BF16),
            pltpu.VMEM((3 * pixels, 2 * channels), F32),
            pltpu.VMEM((2, 2 * pixels, 2 * channels), BF16),
            pltpu.VMEM((2 * pixels, 4 * outputs), F32),
            pltpu.VMEM((2, 2 * frames * outputs, width), BF16),
            pltpu.SemaphoreType.DMA((2,)),
        ],
        compiler_params=pltpu.CompilerParams(vmem_limit_bytes=UP_VMEM),
        cost_estimate=pl.CostEstimate(
            flops=8 * pixels * 4 * channels * outputs * 2, bytes_accessed=2**23, transcendentals=0
        ),
        name="up",
    )(*inputs)
    return jnp.swapaxes(out, 2, 3)


def solution(mesh):
    placed = P("parts", ROWS, None, None)
    return jax.shard_map(
        on_device,
        mesh=mesh,
        in_specs=(placed,) * 3 + (P(),) * 8,
        out_specs=placed,
        check_vma=False,
    )
```

```python
import functools

import jax
import jax.numpy as jnp
from jax import lax
from jax.experimental import pallas as pl
from jax.experimental.pallas import tpu as pltpu
from jax.sharding import PartitionSpec as P

GROUPS = 32
ROWS = "rows"
EPSILON = 1e-06
LANES = 128
F32 = jnp.float32
BF16 = jnp.bfloat16
ALL_VMEM = 67043328
CACHED_VMEM = 44 * 2**20
CONV_VMEM = 50 * 2**20
UP_VMEM = 24 * 2**20
VMEM = pl.BlockSpec(memory_space=pltpu.VMEM)
HBM = pl.BlockSpec(memory_space=pltpu.HBM)


def group_matrix(channels, first, flip):
    size = channels // GROUPS
    shape = (LANES, channels) if flip else (channels, LANES)
    lane = lax.broadcasted_iota(jnp.int32, shape, 0 if flip else 1) - first
    channel = lax.broadcasted_iota(jnp.int32, shape, 1 if flip else 0)
    return ((channel >= lane * size) & (channel < lane * size + size) & (lane >= 0)).astype(F32)


def exact_dot(a, b):
    return jnp.dot(a, b, preferred_element_type=F32, precision=lax.Precision.HIGHEST)


def pack_kernel(latent, conv_cache, time_cache, near, sums, sems):
    frames, _, _, channels = latent.shape
    jobs = []
    for n, source in enumerate((latent, conv_cache, time_cache)):
        for t in range(frames):
            jobs.append((source.at[t, 0], near.at[n * frames + t]))
    copies = [pltpu.make_async_copy(a, b, sems.at[i]) for i, (a, b) in enumerate(jobs)]
    for copy in copies:
        copy.start()
    total = jnp.zeros((8, channels), F32)
    square = jnp.zeros((8, channels), F32)
    for t in range(frames):
        copies[t].wait()
        wide = near[t].astype(F32).reshape(-1, 8, channels)
        total = total + jnp.sum(wide, axis=0)
        square = square + jnp.sum(wide * wide, axis=0)
    grouped = exact_dot(total, group_matrix(channels, 0, False))
    grouped = grouped + exact_dot(square, group_matrix(channels, GROUPS, False))
    row = jnp.sum(grouped, axis=0, keepdims=True)
    sums[...] = jnp.broadcast_to(row[None], sums.shape)
    for copy in copies[frames:]:
        copy.wait()


def shifted(value, step):
    length = value.shape[0]
    rolled = pltpu.roll(value, (-step) % length, 0)
    row = lax.broadcasted_iota(jnp.int32, value.shape, 0)
    return jnp.where((row + step >= 0) & (row + step < length), rolled, 0.0)


def inside_image(step):
    row = lax.axis_index(ROWS) + step
    return ((row >= 0) & (row < lax.axis_size(ROWS))).astype(F32)


def row_at(b, own, partner, outer, frame):
    if b == 1:
        return own[frame]
    even = lax.axis_index(ROWS) % 2 == 0
    first, second = (outer, partner) if b == 0 else (partner, outer)
    return jnp.where(even, first[frame], second[frame])


def start_copies(refs, sems):
    copies = [pltpu.make_async_copy(a, b, sems.at[n]) for n, (a, b) in enumerate(refs)]
    for copy in copies:
        copy.start()
    return copies


def weight_copies(weight_far, weight, taken, sems):
    channels = weight.shape[-1]
    moves = []
    for c in range(3):
        for n, a in enumerate(taken):
            for b in range(3):
                rows = pl.ds(b * channels, channels)
                moves.append((weight_far.at[a, b, c], weight.at[c, n, rows, :]))
    return start_copies(moves, sems)


def tap_sums(copies, taps, weight, acc, shared, single, rows):
    source, target = rows
    for c in range(3):
        for copy in copies[6 * c : 6 * c + 6]:
            copy.wait()
        acc[c] = jnp.dot(taps[...], weight[c, shared], preferred_element_type=F32)
        more = jnp.dot(taps[source, :], weight[c, single], preferred_element_type=F32)
        acc[c, target, :] = acc[c, target, :] + more


def joined_columns(acc, rows):
    return acc[1, rows, :] + shifted(acc[0, rows, :], -1) + shifted(acc[2, rows, :], 1)


def cached_kernel(vectors, own, partner, outer, weight_far, out, weight, taps, acc, sems):
    width, channels = own.shape[1:]
    copies = weight_copies(weight_far, weight, (0, 1), sems)
    first, second = pl.ds(0, width), pl.ds(width, width)
    for b in range(3):
        for t, lines in enumerate((first, second)):
            taps[lines, b * channels : (b + 1) * channels] = row_at(b, own, partner, outer, 2 + t)
    tap_sums(copies, taps, weight, acc, 0, 1, (second, first))
    conv_bias = vectors[:, 2 * channels : 3 * channels]
    for t, lines in enumerate((first, second)):
        latent = own[t].astype(F32)
        out[t] = joined_columns(acc, lines) + conv_bias + latent
        out[2 + t] = latent


def conv_kernel(entries, stats, vectors, own, partner, outer, weight_far, out, weight, taps, acc, sems):
    width, channels = own.shape[1:]
    copies = weight_copies(weight_far, weight, (1, 2), sems)
    gain, shift = (vectors[:, n * channels : (n + 1) * channels] for n in range(2))
    total = jnp.sum(stats[:, 0, :], axis=0, keepdims=True)
    total = jnp.broadcast_to(total, (8, LANES))
    center = exact_dot(total, group_matrix(channels, 0, True))[:1] / entries
    spread = exact_dot(total, group_matrix(channels, GROUPS, True))[:1] / entries
    spread = spread - center * center
    scale = lax.rsqrt(spread + EPSILON) * gain
    first, second = pl.ds(0, width), pl.ds(width, width)
    for b in range(3):
        inside = inside_image(b - 1)
        for t, lines in enumerate((first, second)):
            value = own[2 + t] if b == 1 else row_at(b, own, partner, outer, t).astype(F32)
            value = (value - center) * scale + shift
            value = value / (1.0 + jnp.exp(-value)) * inside
            taps[lines, b * channels : (b + 1) * channels] = value.astype(BF16)
    tap_sums(copies, taps, weight, acc, 1, 0, (first, second))
    for t, lines in enumerate((first, second)):
        out[t] = (joined_columns(acc, lines) + own[t]).astype(BF16)


def mix_kernel(own, partner, outer, block, vectors, time_weight, doubled, partial, taps):
    frames, width, channels = block.shape
    time_bias = vectors[:, 3 * channels : 5 * channels]
    joined = [own[4], own[5], block[0], block[1]]
    for t in range(2):
        for a in range(3):
            taps[pl.ds(t * width, width), a * channels : (a + 1) * channels] = joined[t + a]
    weights = time_weight[...].reshape(3 * channels, 2 * channels)
    mixed = jnp.dot(taps[...], weights, preferred_element_type=F32) + time_bias
    for t in range(2):
        for k in range(2):
            lines = pl.ds((2 * t + k) * width, width)
            part = mixed[t * width : (t + 1) * width, k * channels : (k + 1) * channels]
            doubled[lines, :] = part.astype(BF16)
    for n, r in enumerate((0, 2)):
        for t in range(2):
            cached = row_at(r, own, partner, outer, 4 + t)
            taps[pl.ds(n * width, width), t * channels : (t + 1) * channels] = cached
    first = taps[:, : 2 * channels]
    partial[0] = jnp.dot(first, weights[: 2 * channels], preferred_element_type=F32) + time_bias
    second = taps[:, channels : 2 * channels]
    partial[1] = jnp.dot(second, weights[:channels], preferred_element_type=F32) + time_bias


def up_kernel(
    doubled,
    partial,
    block_partner,
    block_outer,
    vectors,
    time_weight,
    up_weight,
    far_out,
    out,
    taps,
    up_taps,
    lifted,
    turned,
    sems,
):
    frames, width, channels = block_outer.shape
    outputs = out.shape[-2]
    up_bias = vectors[:, 5 * channels :]
    copies = []
    for n, r in enumerate((0, 2)):
        for t in range(2):
            item = row_at(r, None, block_partner, block_outer, t)
            taps[pl.ds(n * width, width), t * channels : (t + 1) * channels] = item
    for p in range(2):
        up_taps[p, :, (1 - p) * channels : (2 - p) * channels] = doubled[...]
    first = jnp.dot(taps[:, :channels], time_weight[2], preferred_element_type=F32)
    weights = time_weight[...].reshape(3 * channels, 2 * channels)[channels:]
    second = jnp.dot(taps[...], weights, preferred_element_type=F32)
    for t, sums in enumerate((first, second)):
        for n, step in enumerate((-1, 1)):
            rows = slice(n * width, (n + 1) * width)
            value = ((sums[rows] + partial[t, rows, :]) * inside_image(step)).astype(BF16)
            for k in range(2):
                lines = pl.ds((2 * t + k) * width, width)
                part = value[:, k * channels : (k + 1) * channels]
                up_taps[n, lines, n * channels : (n + 1) * channels] = part

    lane = lax.broadcasted_iota(jnp.int32, (width, 2 * outputs), 1)
    low = lax.broadcasted_iota(jnp.int32, (width, 2 * width), 0)
    high = lax.broadcasted_iota(jnp.int32, (width, 2 * width), 1)
    spread_out = [(high == 2 * low + q).astype(F32).astype(BF16) for q in range(2)]
    for p in range(2):
        lifted[...] = dot_nt(up_taps[p], up_weight[p])
        for f in range(2 * frames):
            lines = pl.ds(f * width, width)
            inner, outer = lifted[lines, : 2 * outputs], lifted[lines, 2 * outputs :]
            outer = jnp.where(lane < outputs, shifted(outer, -1), shifted(outer, 1))
            value = (inner + outer + up_bias).T.astype(BF16)
            for q in range(2):
                turned[q, pl.ds(f * outputs, outputs), :] = value[q * outputs : (q + 1) * outputs]
        value = jnp.dot(turned[0], spread_out[0], preferred_element_type=F32)
        value = value + jnp.dot(turned[1], spread_out[1], preferred_element_type=F32)
        out[p] = value.astype(BF16).reshape(2 * frames, outputs, 2 * width)
        copies.append(pltpu.make_async_copy(out.at[p], far_out.at[:, p], sems.at[p]))
        copies[p].start()
    for copy in copies:
        copy.wait()


def dot_nt(a, b):
    return lax.dot_general(a, b, (((1,), (1,)), ((), ())), preferred_element_type=F32)


def subpixel_kernel(up_weight, out):
    outputs, channels = up_weight.shape[2:]
    columns = lambda b: [up_weight[b, c].astype(F32) for c in range(3)]
    first, middle, final = columns(0), columns(1), columns(2)
    add = lambda u, v: [x + y for x, y in zip(u, v)]
    by_row = ((first, add(middle, final)), (add(first, middle), final))
    for p in range(2):
        for j in range(2):
            v = by_row[p][j]
            for n, item in enumerate((v[1] + v[2], v[0] + v[1], v[0], v[2])):
                rows = pl.ds(n * outputs, outputs)
                out[p, rows, j * channels : (j + 1) * channels] = item.astype(BF16)


def swapped(value):
    devices = lax.axis_size(ROWS)
    across = [(i, i - 1 if i % 2 == 0 else i + 1) for i in range(devices)]
    across = [(i, j) for i, j in across if 0 <= j < devices]
    outer = lax.ppermute(value, ROWS, across)
    return lax.ppermute(value, ROWS, [(i, i ^ 1) for i in range(devices)]), outer


def on_device(
    latent,
    conv_cache,
    time_cache,
    norm_gain,
    norm_shift,
    conv_weight,
    conv_bias,
    time_weight,
    time_bias,
    up_weight,
    up_bias,
):
    frames, row_count, width, channels = latent.shape
    outputs = up_weight.shape[-1]
    devices = lax.axis_size(ROWS)
    near, sums = pl.pallas_call(
        pack_kernel,
        out_shape=(
            jax.ShapeDtypeStruct((3 * frames, width, channels), BF16),
            jax.ShapeDtypeStruct((devices, 1, LANES), F32),
        ),
        in_specs=[HBM] * 3,
        out_specs=(VMEM,) * 2,
        scratch_shapes=[pltpu.SemaphoreType.DMA((3 * frames,))],
        compiler_params=pltpu.CompilerParams(vmem_limit_bytes=ALL_VMEM),
        cost_estimate=pl.CostEstimate(flops=2**21, bytes_accessed=2**21, transcendentals=0),
        name="pack",
    )(latent, conv_cache, time_cache)
    partner, outer = swapped(near)
    stats = lax.all_to_all(sums, ROWS, 0, 0)
    entries = float(frames * row_count * devices * width * (channels // GROUPS))
    subpixel = pl.pallas_call(
        subpixel_kernel,
        out_shape=jax.ShapeDtypeStruct((2, 4 * outputs, 2 * channels), BF16),
        in_specs=[VMEM],
        out_specs=VMEM,
        compiler_params=pltpu.CompilerParams(vmem_limit_bytes=12 * 2**20),
        cost_estimate=pl.CostEstimate(flops=2**21, bytes_accessed=2**24, transcendentals=0),
        name="subpixel",
    )(jnp.swapaxes(up_weight, 2, 3))
    vectors = jnp.concatenate([norm_gain, norm_shift, conv_bias, time_bias, up_bias, up_bias])
    vectors = vectors.reshape(1, -1)
    pixels = frames * width
    flops = pixels * 27 * channels * channels
    scratch = [
        pltpu.VMEM((3, 2, 3 * channels, channels), BF16),
        pltpu.VMEM((pixels, 3 * channels), BF16),
        pltpu.VMEM((3, pixels, channels), F32),
        pltpu.SemaphoreType.DMA((18,)),
    ]
    base = pl.pallas_call(
        cached_kernel,
        out_shape=jax.ShapeDtypeStruct((2 * frames, width, channels), F32),
        in_specs=[VMEM] * 4 + [HBM],
        out_specs=VMEM,
        scratch_shapes=scratch,
        compiler_params=pltpu.CompilerParams(vmem_limit_bytes=CACHED_VMEM),
        cost_estimate=pl.CostEstimate(flops=flops, bytes_accessed=2**23, transcendentals=0),
        name="cached",
    )(vectors, near, partner, outer, conv_weight)
    block = pl.pallas_call(
        functools.partial(conv_kernel, entries),
        out_shape=jax.ShapeDtypeStruct((frames, width, channels), BF16),
        in_specs=[VMEM] * 5 + [HBM],
        out_specs=VMEM,
        scratch_shapes=scratch,
        compiler_params=pltpu.CompilerParams(vmem_limit_bytes=CONV_VMEM),
        cost_estimate=pl.CostEstimate(flops=flops, bytes_accessed=2**23, transcendentals=2**18),
        name="conv",
    )(stats, vectors, base, partner, outer, conv_weight)
    block_partner, block_outer = swapped(block)
    doubled, partial = pl.pallas_call(
        mix_kernel,
        out_shape=(
            jax.ShapeDtypeStruct((2 * pixels, channels), BF16),
            jax.ShapeDtypeStruct((frames, pixels, 2 * channels), F32),
        ),
        in_specs=[VMEM] * 6,
        out_specs=(VMEM, VMEM),
        scratch_shapes=[pltpu.VMEM((pixels, 3 * channels), BF16)],
        compiler_params=pltpu.CompilerParams(vmem_limit_bytes=16 * 2**20),
        cost_estimate=pl.CostEstimate(flops=2**21, bytes_accessed=2**22, transcendentals=0),
        name="mix",
    )(near, partner, outer, block, vectors, time_weight)
    out = pl.pallas_call(
        up_kernel,
        out_shape=jax.ShapeDtypeStruct((2 * frames, 2, outputs, 2 * width), BF16),
        in_specs=[VMEM] * 7,
        out_specs=HBM,
        scratch_shapes=[
            pltpu.VMEM((2, 2 * frames, outputs, 2 * width), BF16),
            pltpu.VMEM((pixels, 2 * channels), BF16),
            pltpu.VMEM((2, 2 * pixels, 2 * channels), BF16),
            pltpu.VMEM((2 * pixels, 4 * outputs), F32),
            pltpu.VMEM((2, 2 * frames * outputs, width), BF16),
            pltpu.SemaphoreType.DMA((2,)),
        ],
        compiler_params=pltpu.CompilerParams(vmem_limit_bytes=UP_VMEM),
        cost_estimate=pl.CostEstimate(
            flops=8 * pixels * 4 * channels * outputs * 2, bytes_accessed=2**23, transcendentals=0
        ),
        name="up",
    )(doubled, partial, block_partner, block_outer, vectors, time_weight, subpixel)
    return jnp.swapaxes(out, 2, 3)


def solution(mesh):
    placed = P("parts", ROWS, None, None)
    return jax.shard_map(
        on_device,
        mesh=mesh,
        in_specs=(placed,) * 3 + (P(),) * 8,
        out_specs=placed,
        check_vma=False,
    )
```

```python
import functools

import jax
import jax.numpy as jnp
from jax import lax
from jax.experimental import pallas as pl
from jax.experimental.pallas import tpu as pltpu
from jax.sharding import PartitionSpec as P

GROUPS = 32
ROWS = "rows"
EPSILON = 1e-06
LANES = 128
F32 = jnp.float32
BF16 = jnp.bfloat16
ALL_VMEM = 67043328
CACHED_VMEM = 44 * 2**20
CONV_VMEM = 50 * 2**20
UP_VMEM = 24 * 2**20
VMEM = pl.BlockSpec(memory_space=pltpu.VMEM)
HBM = pl.BlockSpec(memory_space=pltpu.HBM)


def group_matrix(channels, first, flip):
    size = channels // GROUPS
    shape = (LANES, channels) if flip else (channels, LANES)
    lane = lax.broadcasted_iota(jnp.int32, shape, 0 if flip else 1) - first
    channel = lax.broadcasted_iota(jnp.int32, shape, 1 if flip else 0)
    return ((channel >= lane * size) & (channel < lane * size + size) & (lane >= 0)).astype(F32)


def exact_dot(a, b):
    return jnp.dot(a, b, preferred_element_type=F32, precision=lax.Precision.HIGHEST)


def pack_kernel(latent, conv_cache, time_cache, near, sums, sems):
    frames, _, _, channels = latent.shape
    jobs = []
    for n, source in enumerate((latent, conv_cache, time_cache)):
        for t in range(frames):
            jobs.append((source.at[t, 0], near.at[n * frames + t]))
    copies = [pltpu.make_async_copy(a, b, sems.at[i]) for i, (a, b) in enumerate(jobs)]
    for copy in copies:
        copy.start()
    total = jnp.zeros((8, channels), F32)
    square = jnp.zeros((8, channels), F32)
    for t in range(frames):
        copies[t].wait()
        wide = near[t].astype(F32).reshape(-1, 8, channels)
        total = total + jnp.sum(wide, axis=0)
        square = square + jnp.sum(wide * wide, axis=0)
    grouped = exact_dot(total, group_matrix(channels, 0, False))
    grouped = grouped + exact_dot(square, group_matrix(channels, GROUPS, False))
    row = jnp.sum(grouped, axis=0, keepdims=True)
    sums[...] = jnp.broadcast_to(row[None], sums.shape)
    for copy in copies[frames:]:
        copy.wait()


def shifted(value, step):
    length = value.shape[0]
    rolled = pltpu.roll(value, (-step) % length, 0)
    row = lax.broadcasted_iota(jnp.int32, value.shape, 0)
    return jnp.where((row + step >= 0) & (row + step < length), rolled, 0.0)


def inside_image(step):
    row = lax.axis_index(ROWS) + step
    return ((row >= 0) & (row < lax.axis_size(ROWS))).astype(F32)


def row_at(b, own, partner, outer, frame):
    if b == 1:
        return own[frame]
    even = lax.axis_index(ROWS) % 2 == 0
    first, second = (outer, partner) if b == 0 else (partner, outer)
    return jnp.where(even, first[frame], second[frame])


def start_copies(refs, sems):
    copies = [pltpu.make_async_copy(a, b, sems.at[n]) for n, (a, b) in enumerate(refs)]
    for copy in copies:
        copy.start()
    return copies


def weight_copies(weight_far, weight, taken, sems):
    channels = weight.shape[-1]
    moves = []
    for c in range(3):
        for n, a in enumerate(taken):
            for b in range(3):
                rows = pl.ds(b * channels, channels)
                moves.append((weight_far.at[a, b, c], weight.at[c, n, rows, :]))
    return start_copies(moves, sems)


def tap_sums(copies, taps, weight, acc, shared, single, rows):
    source, target = rows
    for c in range(3):
        for copy in copies[6 * c : 6 * c + 6]:
            copy.wait()
        acc[c] = jnp.dot(taps[...], weight[c, shared], preferred_element_type=F32)
        more = jnp.dot(taps[source, :], weight[c, single], preferred_element_type=F32)
        acc[c, target, :] = acc[c, target, :] + more


def joined_columns(acc, rows):
    return acc[1, rows, :] + shifted(acc[0, rows, :], -1) + shifted(acc[2, rows, :], 1)


def cached_kernel(vectors, own, partner, outer, weight_far, out, weight, taps, acc, sems):
    width, channels = own.shape[1:]
    copies = weight_copies(weight_far, weight, (0, 1), sems)
    first, second = pl.ds(0, width), pl.ds(width, width)
    for b in range(3):
        for t, lines in enumerate((first, second)):
            taps[lines, b * channels : (b + 1) * channels] = row_at(b, own, partner, outer, 2 + t)
    tap_sums(copies, taps, weight, acc, 0, 1, (second, first))
    conv_bias = vectors[:, 2 * channels : 3 * channels]
    for t, lines in enumerate((first, second)):
        latent = own[t].astype(F32)
        out[t] = joined_columns(acc, lines) + conv_bias + latent
        out[2 + t] = latent


def conv_kernel(entries, stats, vectors, own, partner, outer, weight_far, out, weight, taps, acc, sems):
    width, channels = own.shape[1:]
    copies = weight_copies(weight_far, weight, (1, 2), sems)
    gain, shift = (vectors[:, n * channels : (n + 1) * channels] for n in range(2))
    total = jnp.sum(stats[:, 0, :], axis=0, keepdims=True)
    total = jnp.broadcast_to(total, (8, LANES))
    center = exact_dot(total, group_matrix(channels, 0, True))[:1] / entries
    spread = exact_dot(total, group_matrix(channels, GROUPS, True))[:1] / entries
    spread = spread - center * center
    scale = lax.rsqrt(spread + EPSILON) * gain
    first, second = pl.ds(0, width), pl.ds(width, width)
    for b in range(3):
        inside = inside_image(b - 1)
        for t, lines in enumerate((first, second)):
            value = own[2 + t] if b == 1 else row_at(b, own, partner, outer, t).astype(F32)
            value = (value - center) * scale + shift
            value = value / (1.0 + jnp.exp(-value)) * inside
            taps[lines, b * channels : (b + 1) * channels] = value.astype(BF16)
    tap_sums(copies, taps, weight, acc, 1, 0, (first, second))
    for t, lines in enumerate((first, second)):
        out[t] = (joined_columns(acc, lines) + own[t]).astype(BF16)


def mix_kernel(own, partner, outer, block, vectors, time_weight, up_weight, own_lift, partial, taps, doubled):
    frames, width, channels = block.shape
    time_bias = vectors[:, 3 * channels : 5 * channels]
    joined = [own[4], own[5], block[0], block[1]]
    for t in range(2):
        for a in range(3):
            taps[pl.ds(t * width, width), a * channels : (a + 1) * channels] = joined[t + a]
    weights = time_weight[...].reshape(3 * channels, 2 * channels)
    mixed = jnp.dot(taps[...], weights, preferred_element_type=F32) + time_bias
    for t in range(2):
        for k in range(2):
            lines = pl.ds((2 * t + k) * width, width)
            part = mixed[t * width : (t + 1) * width, k * channels : (k + 1) * channels]
            doubled[lines, :] = part.astype(BF16)
    for p in range(2):
        own_lift[p] = dot_nt(doubled[...], up_weight[p, :, (1 - p) * channels : (2 - p) * channels])
    for n, r in enumerate((0, 2)):
        for t in range(2):
            cached = row_at(r, own, partner, outer, 4 + t)
            taps[pl.ds(n * width, width), t * channels : (t + 1) * channels] = cached
    first = taps[:, : 2 * channels]
    partial[0] = jnp.dot(first, weights[: 2 * channels], preferred_element_type=F32) + time_bias
    second = taps[:, channels : 2 * channels]
    partial[1] = jnp.dot(second, weights[:channels], preferred_element_type=F32) + time_bias


def up_kernel(
    own_lift,
    partial,
    block_partner,
    block_outer,
    vectors,
    time_weight,
    up_weight,
    far_out,
    out,
    taps,
    up_taps,
    lifted,
    turned,
    sems,
):
    frames, width, channels = block_outer.shape
    outputs = out.shape[-2]
    up_bias = vectors[:, 5 * channels :]
    copies = []
    for n, r in enumerate((0, 2)):
        for t in range(2):
            item = row_at(r, None, block_partner, block_outer, t)
            taps[pl.ds(n * width, width), t * channels : (t + 1) * channels] = item
    first = jnp.dot(taps[:, :channels], time_weight[2], preferred_element_type=F32)
    weights = time_weight[...].reshape(3 * channels, 2 * channels)[channels:]
    second = jnp.dot(taps[...], weights, preferred_element_type=F32)
    for t, sums in enumerate((first, second)):
        for n, step in enumerate((-1, 1)):
            rows = slice(n * width, (n + 1) * width)
            value = ((sums[rows] + partial[t, rows, :]) * inside_image(step)).astype(BF16)
            for k in range(2):
                lines = pl.ds((2 * t + k) * width, width)
                part = value[:, k * channels : (k + 1) * channels]
                up_taps[n, lines, :] = part

    lane = lax.broadcasted_iota(jnp.int32, (width, 2 * outputs), 1)
    low = lax.broadcasted_iota(jnp.int32, (width, 2 * width), 0)
    high = lax.broadcasted_iota(jnp.int32, (width, 2 * width), 1)
    spread_out = [(high == 2 * low + q).astype(F32).astype(BF16) for q in range(2)]
    for p in range(2):
        lifted[...] = dot_nt(up_taps[p], up_weight[p, :, p * channels : (p + 1) * channels])
        for f in range(2 * frames):
            lines = pl.ds(f * width, width)
            both = lifted[lines, :] + own_lift[p, lines, :]
            inner, outer = both[:, : 2 * outputs], both[:, 2 * outputs :]
            outer = jnp.where(lane < outputs, shifted(outer, -1), shifted(outer, 1))
            value = (inner + outer + up_bias).T.astype(BF16)
            for q in range(2):
                turned[q, pl.ds(f * outputs, outputs), :] = value[q * outputs : (q + 1) * outputs]
        value = jnp.dot(turned[0], spread_out[0], preferred_element_type=F32)
        value = value + jnp.dot(turned[1], spread_out[1], preferred_element_type=F32)
        out[p] = value.astype(BF16).reshape(2 * frames, outputs, 2 * width)
        copies.append(pltpu.make_async_copy(out.at[p], far_out.at[:, p], sems.at[p]))
        copies[p].start()
    for copy in copies:
        copy.wait()


def dot_nt(a, b):
    return lax.dot_general(a, b, (((1,), (1,)), ((), ())), preferred_element_type=F32)


def subpixel_kernel(up_weight, out):
    outputs, channels = up_weight.shape[2:]
    columns = lambda b: [up_weight[b, c].astype(F32) for c in range(3)]
    first, middle, final = columns(0), columns(1), columns(2)
    add = lambda u, v: [x + y for x, y in zip(u, v)]
    by_row = ((first, add(middle, final)), (add(first, middle), final))
    for p in range(2):
        for j in range(2):
            v = by_row[p][j]
            for n, item in enumerate((v[1] + v[2], v[0] + v[1], v[0], v[2])):
                rows = pl.ds(n * outputs, outputs)
                out[p, rows, j * channels : (j + 1) * channels] = item.astype(BF16)


def swapped(value):
    devices = lax.axis_size(ROWS)
    across = [(i, i - 1 if i % 2 == 0 else i + 1) for i in range(devices)]
    across = [(i, j) for i, j in across if 0 <= j < devices]
    outer = lax.ppermute(value, ROWS, across)
    return lax.ppermute(value, ROWS, [(i, i ^ 1) for i in range(devices)]), outer


def on_device(
    latent,
    conv_cache,
    time_cache,
    norm_gain,
    norm_shift,
    conv_weight,
    conv_bias,
    time_weight,
    time_bias,
    up_weight,
    up_bias,
):
    frames, row_count, width, channels = latent.shape
    outputs = up_weight.shape[-1]
    devices = lax.axis_size(ROWS)
    near, sums = pl.pallas_call(
        pack_kernel,
        out_shape=(
            jax.ShapeDtypeStruct((3 * frames, width, channels), BF16),
            jax.ShapeDtypeStruct((devices, 1, LANES), F32),
        ),
        in_specs=[HBM] * 3,
        out_specs=(VMEM,) * 2,
        scratch_shapes=[pltpu.SemaphoreType.DMA((3 * frames,))],
        compiler_params=pltpu.CompilerParams(vmem_limit_bytes=ALL_VMEM),
        cost_estimate=pl.CostEstimate(flops=2**21, bytes_accessed=2**21, transcendentals=0),
        name="pack",
    )(latent, conv_cache, time_cache)
    partner, outer = swapped(near)
    stats = lax.all_to_all(sums, ROWS, 0, 0)
    entries = float(frames * row_count * devices * width * (channels // GROUPS))
    subpixel = pl.pallas_call(
        subpixel_kernel,
        out_shape=jax.ShapeDtypeStruct((2, 4 * outputs, 2 * channels), BF16),
        in_specs=[VMEM],
        out_specs=VMEM,
        compiler_params=pltpu.CompilerParams(vmem_limit_bytes=12 * 2**20),
        cost_estimate=pl.CostEstimate(flops=2**21, bytes_accessed=2**24, transcendentals=0),
        name="subpixel",
    )(jnp.swapaxes(up_weight, 2, 3))
    vectors = jnp.concatenate([norm_gain, norm_shift, conv_bias, time_bias, up_bias, up_bias])
    vectors = vectors.reshape(1, -1)
    pixels = frames * width
    flops = pixels * 27 * channels * channels
    scratch = [
        pltpu.VMEM((3, 2, 3 * channels, channels), BF16),
        pltpu.VMEM((pixels, 3 * channels), BF16),
        pltpu.VMEM((3, pixels, channels), F32),
        pltpu.SemaphoreType.DMA((18,)),
    ]
    base = pl.pallas_call(
        cached_kernel,
        out_shape=jax.ShapeDtypeStruct((2 * frames, width, channels), F32),
        in_specs=[VMEM] * 4 + [HBM],
        out_specs=VMEM,
        scratch_shapes=scratch,
        compiler_params=pltpu.CompilerParams(vmem_limit_bytes=CACHED_VMEM),
        cost_estimate=pl.CostEstimate(flops=flops, bytes_accessed=2**23, transcendentals=0),
        name="cached",
    )(vectors, near, partner, outer, conv_weight)
    block = pl.pallas_call(
        functools.partial(conv_kernel, entries),
        out_shape=jax.ShapeDtypeStruct((frames, width, channels), BF16),
        in_specs=[VMEM] * 5 + [HBM],
        out_specs=VMEM,
        scratch_shapes=scratch,
        compiler_params=pltpu.CompilerParams(vmem_limit_bytes=CONV_VMEM),
        cost_estimate=pl.CostEstimate(flops=flops, bytes_accessed=2**23, transcendentals=2**18),
        name="conv",
    )(stats, vectors, base, partner, outer, conv_weight)
    block_partner, block_outer = swapped(block)
    own_lift, partial = pl.pallas_call(
        mix_kernel,
        out_shape=(
            jax.ShapeDtypeStruct((2, 2 * pixels, 4 * outputs), F32),
            jax.ShapeDtypeStruct((frames, pixels, 2 * channels), F32),
        ),
        in_specs=[VMEM] * 7,
        out_specs=(VMEM, VMEM),
        scratch_shapes=[pltpu.VMEM((pixels, 3 * channels), BF16), pltpu.VMEM((2 * pixels, channels), BF16)],
        compiler_params=pltpu.CompilerParams(vmem_limit_bytes=16 * 2**20),
        cost_estimate=pl.CostEstimate(flops=2**21, bytes_accessed=2**22, transcendentals=0),
        name="mix",
    )(near, partner, outer, block, vectors, time_weight, subpixel)
    out = pl.pallas_call(
        up_kernel,
        out_shape=jax.ShapeDtypeStruct((2 * frames, 2, outputs, 2 * width), BF16),
        in_specs=[VMEM] * 7,
        out_specs=HBM,
        scratch_shapes=[
            pltpu.VMEM((2, 2 * frames, outputs, 2 * width), BF16),
            pltpu.VMEM((pixels, 2 * channels), BF16),
            pltpu.VMEM((2, 2 * pixels, channels), BF16),
            pltpu.VMEM((2 * pixels, 4 * outputs), F32),
            pltpu.VMEM((2, 2 * frames * outputs, width), BF16),
            pltpu.SemaphoreType.DMA((2,)),
        ],
        compiler_params=pltpu.CompilerParams(vmem_limit_bytes=UP_VMEM),
        cost_estimate=pl.CostEstimate(
            flops=8 * pixels * 4 * channels * outputs * 2, bytes_accessed=2**23, transcendentals=0
        ),
        name="up",
    )(own_lift, partial, block_partner, block_outer, vectors, time_weight, subpixel)
    return jnp.swapaxes(out, 2, 3)


def solution(mesh):
    placed = P("parts", ROWS, None, None)
    return jax.shard_map(
        on_device,
        mesh=mesh,
        in_specs=(placed,) * 3 + (P(),) * 8,
        out_specs=placed,
        check_vma=False,
    )
```

```python
import functools

import jax
import jax.numpy as jnp
from jax import lax
from jax.experimental import pallas as pl
from jax.experimental.pallas import tpu as pltpu
from jax.sharding import PartitionSpec as P

GROUPS = 32
ROWS = "rows"
EPSILON = 1e-06
LANES = 128
F32 = jnp.float32
BF16 = jnp.bfloat16
ALL_VMEM = 67043328
CACHED_VMEM = 44 * 2**20
CONV_VMEM = 50 * 2**20
UP_VMEM = 24 * 2**20
VMEM = pl.BlockSpec(memory_space=pltpu.VMEM)
HBM = pl.BlockSpec(memory_space=pltpu.HBM)


def group_matrix(channels, first, flip):
    size = channels // GROUPS
    shape = (LANES, channels) if flip else (channels, LANES)
    lane = lax.broadcasted_iota(jnp.int32, shape, 0 if flip else 1) - first
    channel = lax.broadcasted_iota(jnp.int32, shape, 1 if flip else 0)
    return ((channel >= lane * size) & (channel < lane * size + size) & (lane >= 0)).astype(F32)


def exact_dot(a, b):
    return jnp.dot(a, b, preferred_element_type=F32, precision=lax.Precision.HIGHEST)


def pack_kernel(latent, conv_cache, time_cache, near_far, sums, near, sems):
    frames, _, _, channels = latent.shape
    copies, onward = [], []
    for n, source in enumerate((latent, conv_cache, time_cache)):
        for t in range(frames):
            i = n * frames + t
            copies.append(pltpu.make_async_copy(source.at[t, 0], near.at[i], sems.at[0, i]))
            onward.append(pltpu.make_async_copy(near.at[i], near_far.at[i], sems.at[1, i]))
    for copy in copies:
        copy.start()
    for copy, after in zip(copies, onward):
        copy.wait()
        after.start()
    total = jnp.zeros((8, channels), F32)
    square = jnp.zeros((8, channels), F32)
    for t in range(frames):
        wide = near[t].astype(F32).reshape(-1, 8, channels)
        total = total + jnp.sum(wide, axis=0)
        square = square + jnp.sum(wide * wide, axis=0)
    grouped = exact_dot(total, group_matrix(channels, 0, False))
    grouped = grouped + exact_dot(square, group_matrix(channels, GROUPS, False))
    row = jnp.sum(grouped, axis=0, keepdims=True)
    sums[...] = jnp.broadcast_to(row[None], sums.shape)
    for copy in onward:
        copy.wait()


def shifted(value, step):
    length = value.shape[0]
    rolled = pltpu.roll(value, (-step) % length, 0)
    row = lax.broadcasted_iota(jnp.int32, value.shape, 0)
    return jnp.where((row + step >= 0) & (row + step < length), rolled, 0.0)


def inside_image(step):
    row = lax.axis_index(ROWS) + step
    return ((row >= 0) & (row < lax.axis_size(ROWS))).astype(F32)


def row_at(b, own, partner, outer, frame):
    if b == 1:
        return own[frame]
    even = lax.axis_index(ROWS) % 2 == 0
    first, second = (outer, partner) if b == 0 else (partner, outer)
    return jnp.where(even, first[frame], second[frame])


def start_copies(refs, sems):
    copies = [pltpu.make_async_copy(a, b, sems.at[n]) for n, (a, b) in enumerate(refs)]
    for copy in copies:
        copy.start()
    return copies


def weight_copies(weight_far, weight, taken, sems):
    channels = weight.shape[-1]
    moves = []
    for c in range(3):
        for n, a in enumerate(taken):
            for b in range(3):
                rows = pl.ds(b * channels, channels)
                moves.append((weight_far.at[a, b, c], weight.at[c, n, rows, :]))
    return start_copies(moves, sems)


def tap_sums(copies, taps, weight, acc, shared, single, rows):
    source, target = rows
    for c in range(3):
        for copy in copies[6 * c : 6 * c + 6]:
            copy.wait()
        acc[c] = jnp.dot(taps[...], weight[c, shared], preferred_element_type=F32)
        more = jnp.dot(taps[source, :], weight[c, single], preferred_element_type=F32)
        acc[c, target, :] = acc[c, target, :] + more


def joined_columns(acc, rows):
    return acc[1, rows, :] + shifted(acc[0, rows, :], -1) + shifted(acc[2, rows, :], 1)


def cached_kernel(vectors, own, partner, outer, weight_far, out, weight, taps, acc, sems):
    width, channels = own.shape[1:]
    copies = weight_copies(weight_far, weight, (0, 1), sems)
    first, second = pl.ds(0, width), pl.ds(width, width)
    for b in range(3):
        for t, lines in enumerate((first, second)):
            taps[lines, b * channels : (b + 1) * channels] = row_at(b, own, partner, outer, 2 + t)
    tap_sums(copies, taps, weight, acc, 0, 1, (second, first))
    conv_bias = vectors[:, 2 * channels : 3 * channels]
    for t, lines in enumerate((first, second)):
        latent = own[t].astype(F32)
        out[t] = joined_columns(acc, lines) + conv_bias + latent
        out[2 + t] = latent


def conv_kernel(entries, stats, vectors, own, partner, outer, weight_far, out, weight, taps, acc, sems):
    width, channels = own.shape[1:]
    copies = weight_copies(weight_far, weight, (1, 2), sems)
    gain, shift = (vectors[:, n * channels : (n + 1) * channels] for n in range(2))
    total = jnp.sum(stats[:, 0, :], axis=0, keepdims=True)
    total = jnp.broadcast_to(total, (8, LANES))
    center = exact_dot(total, group_matrix(channels, 0, True))[:1] / entries
    spread = exact_dot(total, group_matrix(channels, GROUPS, True))[:1] / entries
    spread = spread - center * center
    scale = lax.rsqrt(spread + EPSILON) * gain
    first, second = pl.ds(0, width), pl.ds(width, width)
    for b in range(3):
        inside = inside_image(b - 1)
        for t, lines in enumerate((first, second)):
            value = own[2 + t] if b == 1 else row_at(b, own, partner, outer, t).astype(F32)
            value = (value - center) * scale + shift
            value = value / (1.0 + jnp.exp(-value)) * inside
            taps[lines, b * channels : (b + 1) * channels] = value.astype(BF16)
    tap_sums(copies, taps, weight, acc, 1, 0, (first, second))
    for t, lines in enumerate((first, second)):
        out[t] = (joined_columns(acc, lines) + own[t]).astype(BF16)


def mix_kernel(own, partner, outer, block, vectors, time_weight, doubled, partial, taps):
    frames, width, channels = block.shape
    time_bias = vectors[:, 3 * channels : 5 * channels]
    joined = [own[4], own[5], block[0], block[1]]
    for t in range(2):
        for a in range(3):
            taps[pl.ds(t * width, width), a * channels : (a + 1) * channels] = joined[t + a]
    weights = time_weight[...].reshape(3 * channels, 2 * channels)
    mixed = jnp.dot(taps[...], weights, preferred_element_type=F32) + time_bias
    for t in range(2):
        for k in range(2):
            lines = pl.ds((2 * t + k) * width, width)
            part = mixed[t * width : (t + 1) * width, k * channels : (k + 1) * channels]
            doubled[lines, :] = part.astype(BF16)
    for n, r in enumerate((0, 2)):
        for t in range(2):
            cached = row_at(r, own, partner, outer, 4 + t)
            taps[pl.ds(n * width, width), t * channels : (t + 1) * channels] = cached
    first = taps[:, : 2 * channels]
    partial[0] = jnp.dot(first, weights[: 2 * channels], preferred_element_type=F32) + time_bias
    second = taps[:, channels : 2 * channels]
    partial[1] = jnp.dot(second, weights[:channels], preferred_element_type=F32) + time_bias


def up_kernel(
    doubled,
    partial,
    block_partner,
    block_outer,
    vectors,
    time_weight,
    up_weight,
    far_out,
    out,
    taps,
    up_taps,
    lifted,
    turned,
    sems,
):
    frames, width, channels = block_outer.shape
    outputs = out.shape[-2]
    up_bias = vectors[:, 5 * channels :]
    copies = []
    for n, r in enumerate((0, 2)):
        for t in range(2):
            item = row_at(r, None, block_partner, block_outer, t)
            taps[pl.ds(n * width, width), t * channels : (t + 1) * channels] = item
    for p in range(2):
        up_taps[p, :, (1 - p) * channels : (2 - p) * channels] = doubled[...]
    first = jnp.dot(taps[:, :channels], time_weight[2], preferred_element_type=F32)
    weights = time_weight[...].reshape(3 * channels, 2 * channels)[channels:]
    second = jnp.dot(taps[...], weights, preferred_element_type=F32)
    for t, sums in enumerate((first, second)):
        for n, step in enumerate((-1, 1)):
            rows = slice(n * width, (n + 1) * width)
            value = ((sums[rows] + partial[t, rows, :]) * inside_image(step)).astype(BF16)
            for k in range(2):
                lines = pl.ds((2 * t + k) * width, width)
                part = value[:, k * channels : (k + 1) * channels]
                up_taps[n, lines, n * channels : (n + 1) * channels] = part

    lane = lax.broadcasted_iota(jnp.int32, (width, 2 * outputs), 1)
    low = lax.broadcasted_iota(jnp.int32, (width, 2 * width), 0)
    high = lax.broadcasted_iota(jnp.int32, (width, 2 * width), 1)
    spread_out = [(high == 2 * low + q).astype(F32).astype(BF16) for q in range(2)]
    for p in range(2):
        lifted[...] = dot_nt(up_taps[p], up_weight[p])
        for f in range(2 * frames):
            lines = pl.ds(f * width, width)
            inner, outer = lifted[lines, : 2 * outputs], lifted[lines, 2 * outputs :]
            outer = jnp.where(lane < outputs, shifted(outer, -1), shifted(outer, 1))
            value = (inner + outer + up_bias).T.astype(BF16)
            for q in range(2):
                turned[q, pl.ds(f * outputs, outputs), :] = value[q * outputs : (q + 1) * outputs]
        value = jnp.dot(turned[0], spread_out[0], preferred_element_type=F32)
        value = value + jnp.dot(turned[1], spread_out[1], preferred_element_type=F32)
        out[p] = value.astype(BF16).reshape(2 * frames, outputs, 2 * width)
        copies.append(pltpu.make_async_copy(out.at[p], far_out.at[:, p], sems.at[p]))
        copies[p].start()
    for copy in copies:
        copy.wait()


def dot_nt(a, b):
    return lax.dot_general(a, b, (((1,), (1,)), ((), ())), preferred_element_type=F32)


def subpixel_kernel(up_weight, out):
    outputs, channels = up_weight.shape[2:]
    columns = lambda b: [up_weight[b, c].astype(F32) for c in range(3)]
    first, middle, final = columns(0), columns(1), columns(2)
    add = lambda u, v: [x + y for x, y in zip(u, v)]
    by_row = ((first, add(middle, final)), (add(first, middle), final))
    for p in range(2):
        for j in range(2):
            v = by_row[p][j]
            for n, item in enumerate((v[1] + v[2], v[0] + v[1], v[0], v[2])):
                rows = pl.ds(n * outputs, outputs)
                out[p, rows, j * channels : (j + 1) * channels] = item.astype(BF16)


def swapped(value):
    devices = lax.axis_size(ROWS)
    across = [(i, i - 1 if i % 2 == 0 else i + 1) for i in range(devices)]
    across = [(i, j) for i, j in across if 0 <= j < devices]
    outer = lax.ppermute(value, ROWS, across)
    return lax.ppermute(value, ROWS, [(i, i ^ 1) for i in range(devices)]), outer


def on_device(
    latent,
    conv_cache,
    time_cache,
    norm_gain,
    norm_shift,
    conv_weight,
    conv_bias,
    time_weight,
    time_bias,
    up_weight,
    up_bias,
):
    frames, row_count, width, channels = latent.shape
    outputs = up_weight.shape[-1]
    devices = lax.axis_size(ROWS)
    near, sums = pl.pallas_call(
        pack_kernel,
        out_shape=(
            jax.ShapeDtypeStruct((3 * frames, width, channels), BF16),
            jax.ShapeDtypeStruct((devices, 1, LANES), F32),
        ),
        in_specs=[HBM] * 3,
        out_specs=(HBM, VMEM),
        scratch_shapes=[
            pltpu.VMEM((3 * frames, width, channels), BF16),
            pltpu.SemaphoreType.DMA((2, 3 * frames)),
        ],
        compiler_params=pltpu.CompilerParams(vmem_limit_bytes=ALL_VMEM),
        cost_estimate=pl.CostEstimate(flops=2**21, bytes_accessed=2**21, transcendentals=0),
        name="pack",
    )(latent, conv_cache, time_cache)
    partner, outer = swapped(near)
    stats = lax.all_to_all(sums, ROWS, 0, 0)
    entries = float(frames * row_count * devices * width * (channels // GROUPS))
    subpixel = pl.pallas_call(
        subpixel_kernel,
        out_shape=jax.ShapeDtypeStruct((2, 4 * outputs, 2 * channels), BF16),
        in_specs=[VMEM],
        out_specs=VMEM,
        compiler_params=pltpu.CompilerParams(vmem_limit_bytes=12 * 2**20),
        cost_estimate=pl.CostEstimate(flops=2**21, bytes_accessed=2**24, transcendentals=0),
        name="subpixel",
    )(jnp.swapaxes(up_weight, 2, 3))
    vectors = jnp.concatenate([norm_gain, norm_shift, conv_bias, time_bias, up_bias, up_bias])
    vectors = vectors.reshape(1, -1)
    pixels = frames * width
    flops = pixels * 27 * channels * channels
    scratch = [
        pltpu.VMEM((3, 2, 3 * channels, channels), BF16),
        pltpu.VMEM((pixels, 3 * channels), BF16),
        pltpu.VMEM((3, pixels, channels), F32),
        pltpu.SemaphoreType.DMA((18,)),
    ]
    base = pl.pallas_call(
        cached_kernel,
        out_shape=jax.ShapeDtypeStruct((2 * frames, width, channels), F32),
        in_specs=[VMEM] * 4 + [HBM],
        out_specs=VMEM,
        scratch_shapes=scratch,
        compiler_params=pltpu.CompilerParams(vmem_limit_bytes=CACHED_VMEM),
        cost_estimate=pl.CostEstimate(flops=flops, bytes_accessed=2**23, transcendentals=0),
        name="cached",
    )(vectors, near, partner, outer, conv_weight)
    block = pl.pallas_call(
        functools.partial(conv_kernel, entries),
        out_shape=jax.ShapeDtypeStruct((frames, width, channels), BF16),
        in_specs=[VMEM] * 5 + [HBM],
        out_specs=VMEM,
        scratch_shapes=scratch,
        compiler_params=pltpu.CompilerParams(vmem_limit_bytes=CONV_VMEM),
        cost_estimate=pl.CostEstimate(flops=flops, bytes_accessed=2**23, transcendentals=2**18),
        name="conv",
    )(stats, vectors, base, partner, outer, conv_weight)
    block_partner, block_outer = swapped(block)
    doubled, partial = pl.pallas_call(
        mix_kernel,
        out_shape=(
            jax.ShapeDtypeStruct((2 * pixels, channels), BF16),
            jax.ShapeDtypeStruct((frames, pixels, 2 * channels), F32),
        ),
        in_specs=[VMEM] * 6,
        out_specs=(VMEM, VMEM),
        scratch_shapes=[pltpu.VMEM((pixels, 3 * channels), BF16)],
        compiler_params=pltpu.CompilerParams(vmem_limit_bytes=16 * 2**20),
        cost_estimate=pl.CostEstimate(flops=2**21, bytes_accessed=2**22, transcendentals=0),
        name="mix",
    )(near, partner, outer, block, vectors, time_weight)
    out = pl.pallas_call(
        up_kernel,
        out_shape=jax.ShapeDtypeStruct((2 * frames, 2, outputs, 2 * width), BF16),
        in_specs=[VMEM] * 7,
        out_specs=HBM,
        scratch_shapes=[
            pltpu.VMEM((2, 2 * frames, outputs, 2 * width), BF16),
            pltpu.VMEM((pixels, 2 * channels), BF16),
            pltpu.VMEM((2, 2 * pixels, 2 * channels), BF16),
            pltpu.VMEM((2 * pixels, 4 * outputs), F32),
            pltpu.VMEM((2, 2 * frames * outputs, width), BF16),
            pltpu.SemaphoreType.DMA((2,)),
        ],
        compiler_params=pltpu.CompilerParams(vmem_limit_bytes=UP_VMEM),
        cost_estimate=pl.CostEstimate(
            flops=8 * pixels * 4 * channels * outputs * 2, bytes_accessed=2**23, transcendentals=0
        ),
        name="up",
    )(doubled, partial, block_partner, block_outer, vectors, time_weight, subpixel)
    return jnp.swapaxes(out, 2, 3)


def solution(mesh):
    placed = P("parts", ROWS, None, None)
    return jax.shard_map(
        on_device,
        mesh=mesh,
        in_specs=(placed,) * 3 + (P(),) * 8,
        out_specs=placed,
        check_vma=False,
    )
```
